32 devices in a mesh: layer: 8 (over y, x, core), tensor: 4 (over z).
Axes of the slice: x: 2, y: 2, z: 4, core: 2. Of those that a mesh axis runs over, the one named last changes fastest.
Arguments:
- gradient: bfloat16 [8, 1024, 8192], P(None, 'tensor', 'layer'), may hold values from -8 to 8
- row_basis: bfloat16 [8, 1024, 256], P('layer', 'tensor'), may hold values from -0.1875 to 0.1875
- column_basis: bfloat16 [8, 8192, 256], P('layer', 'tensor'), may hold values from -0.0625 to 0.0625
- row_eigen: float32 [8, 256], P('layer'), may hold values from 0.01 to 10
- column_eigen: float32 [8, 256], P('layer'), may hold values from 0.01 to 10
- row_escape: float32 [8], P('layer'), may hold values from 0.02 to 0.2
- column_escape: float32 [8], P('layer'), may hold values from 0.02 to 0.2
Outputs:
- update: bfloat16 [8, 1024, 8192], P(None, 'tensor', 'layer')
The draws below stay inside these ranges and needn't reach their ends.
All inputs are finite; a program needn't handle non-finite values.
Results may differ from the reference program's by a relative error of at most 0.0055.
Values may be sent and summed in bfloat16 or wider, within the bound.
A program may use at most 128 MiB of HBM per device.

```python
import math
import jax
import jax.numpy as jnp
from jax import lax

D = 8192
BLK = 1024
K = 256
LAYERS = 8


def draw_gradient(key, part):
    first, second, third, fourth = jax.random.split(jax.random.fold_in(key, 17), 4)
    noise = jax.random.normal(first, (LAYERS, BLK, D), jnp.float32)
    segment = jnp.exp(jax.random.uniform(third, (LAYERS, 1, D // 64), jnp.float32, math.log(0.4), math.log(2.5)))
    segment = jnp.repeat(segment, 64, axis=2)
    rowscale = jnp.exp(jax.random.uniform(second, (LAYERS, BLK, 1), jnp.float32, math.log(0.5), math.log(2.0)))
    values = rowscale * segment * noise
    return jnp.clip(values, -8.0, 8.0).astype(jnp.bfloat16)


def steps_of(stream_key, extent, shards, smallest, largest):
    factor_of = 1.0
    for dim, blocks in shards:
        heights = jax.random.uniform(jax.random.fold_in(jax.random.fold_in(stream_key, 6), dim), (blocks,), jnp.float32, smallest / len(shards), largest / len(shards))
        factor_of = factor_of * jnp.repeat(jnp.exp(heights), extent[dim] // blocks).reshape((-1,) + (1,) * (len(extent) - 1 - dim))
    return factor_of


def scatter_about(rng, dims, scale, bound, shards=(), dtype=jnp.bfloat16):
    values = jax.random.normal(rng, dims, jnp.float32) * scale
    if len(shards) > 0:
        values = steps_of(rng, dims, shards, -0.22, 0.18) * values
    return jnp.clip(values, min=-bound, max=bound).astype(dtype)


def setup_inputs(seed: int = 0) -> dict:
    keys = jax.random.split(jax.random.key(seed), 8)
    return {
        "gradient": draw_gradient(jax.random.fold_in(keys[7], 71), 0),
        "row_basis": scatter_about(keys[1], (LAYERS, BLK, K), BLK ** -0.5, 0.1875, ((0, 8), (1, 4))),
        "column_basis": scatter_about(keys[2], (LAYERS, D, K), D ** -0.5, 0.0625, ((0, 8), (1, 4))),
        "row_eigen": jnp.clip(jnp.exp(math.log(10.0) - 6.9077553 * jax.random.uniform(keys[3], (LAYERS, K), jnp.float32) ** steps_of(keys[3], (LAYERS, K), ((0, 8),), -0.2, 0.2)), 0.01, 10.0),
        "column_eigen": jnp.clip(jnp.exp(math.log(10.0) - 6.9077553 * jax.random.uniform(keys[4], (LAYERS, K), jnp.float32) ** steps_of(keys[4], (LAYERS, K), ((0, 8),), -0.2, 0.2)), 0.01, 10.0),
        "row_escape": jnp.clip(jnp.exp(math.log(0.2) - 2.3025851 * jax.random.uniform(keys[5], (LAYERS,), jnp.float32) ** steps_of(keys[5], (LAYERS,), ((0, 8),), -0.2, 0.2)), 0.02, 0.2),
        "column_escape": jnp.clip(jnp.exp(math.log(0.2) - 2.3025851 * jax.random.uniform(keys[6], (LAYERS,), jnp.float32) ** steps_of(keys[6], (LAYERS,), ((0, 8),), -0.2, 0.2)), 0.02, 0.2),
    }


def one_layer(operands):
    block_grad, basis_rows, basis_columns, eigen_rows, eigen_columns, escape_rows, escape_columns = operands
    row_base = escape_rows ** (-0.25)
    column_base = escape_columns ** (-0.25)
    row_coef = (eigen_rows + escape_rows) ** (-0.25) - row_base
    column_coef = (eigen_columns + escape_columns) ** (-0.25) - column_base
    projected = jnp.dot(basis_rows.T, block_grad, preferred_element_type=jnp.float32)
    scaled = (row_coef[:, None] * projected).astype(jnp.bfloat16)
    core = jnp.dot(scaled, basis_columns, preferred_element_type=jnp.float32).astype(jnp.bfloat16)
    middle = jnp.dot(block_grad, basis_columns, preferred_element_type=jnp.float32)
    left_factor = ((row_base * middle + jnp.dot(basis_rows, core, preferred_element_type=jnp.float32)) * column_coef[None, :]).astype(jnp.bfloat16)
    raw_update = row_base * column_base * block_grad.astype(jnp.float32)
    raw_update = raw_update + column_base * jnp.dot(basis_rows, scaled, preferred_element_type=jnp.float32)
    raw_update = raw_update + jnp.dot(left_factor, basis_columns.T, preferred_element_type=jnp.float32)
    grad_sq = jnp.sum(jnp.square(block_grad.astype(jnp.float32)))
    update_sq = jnp.sum(jnp.square(raw_update))
    return (raw_update * jnp.sqrt((grad_sq + 1.0) / (update_sq + 1.0))).astype(jnp.bfloat16)

def reference(gradient, row_basis, column_basis, row_eigen, column_eigen, row_escape, column_escape):
    return lax.map(one_layer, (gradient, row_basis, column_basis, row_eigen, column_eigen, row_escape, column_escape))
```

```python
import functools

import jax
import jax.numpy as jnp
from jax import lax
from jax.experimental import pallas as pl
from jax.experimental.pallas import tpu as pltpu
from jax.sharding import PartitionSpec as P

MESH = pl.DeviceIdType.MESH
F32 = jnp.float32
BF16 = jnp.bfloat16


def remote(src, dst, send, recv, axis, index):
    return pltpu.make_async_remote_copy(
        src_ref=src,
        dst_ref=dst,
        send_sem=send,
        recv_sem=recv,
        device_id={axis: index},
        device_id_type=MESH,
    )


def loop(lo, hi, fn):
    def step(i, carry):
        fn(i)
        return carry

    lax.fori_loop(lo, hi, step, 0)


def dot(a, b, dims=((1,), (0,))):
    return lax.dot_general(a, b, (dims, ((), ())), preferred_element_type=F32)


def quarter(x):
    return lax.rsqrt(jnp.sqrt(x))


def lanes(x):
    s = jnp.sum(x * x, axis=0, keepdims=True)
    out = s[:, 0:128]
    for k in range(1, x.shape[1] // 128):
        out = out + s[:, k * 128:(k + 1) * 128]
    return out


def kernel(
    L, T, NP,
    g, u, cols, reig, ceig, resc, cesc,
    raw, factor,
    uall, vall, vline, own, pin, qin, mout, mi, mid, lall, core_in, cb,
    nsend, tile, nin, fsend, fin,
    us, ur, bs, br, vs, vr, xs, xr, ms, mr, ks, kr, ls, lr, ps, pr, qs, qr, ns, nr, fs, fr,
):
    me = lax.axis_index("layer")
    t = lax.axis_index("tensor")
    W = g.shape[2]
    Cr = cols.shape[0]
    B = Cr // W
    BP = B // NP
    PR = Cr // NP
    K = u.shape[1]
    right, lft = t + 1, t - 1
    has_right, has_left = t < T - 1, t > 0
    inner = has_right & has_left
    far = jnp.maximum(t, T - 1 - t)

    barrier = pltpu.get_barrier_semaphore()
    loop(1, L, lambda d: pl.semaphore_signal(
        barrier, inc=1, device_id={"layer": lax.rem(me + d, L)}, device_id_type=MESH))
    loop(1, T, lambda d: pl.semaphore_signal(
        barrier, inc=1, device_id={"tensor": lax.rem(t + d, T)}, device_id_type=MESH))

    row_base = quarter(resc[...])
    column_base = quarter(cesc[...])
    row_coef = quarter(reig[...] + resc[...]) - row_base
    dc = quarter(ceig[...] + cesc[...]) - column_base
    cb[me, 0:1, :] = row_coef * column_base
    cb[me, 1:2, :] = jnp.broadcast_to(row_base * column_base, (1, K))
    cb[me, 2:8, :] = jnp.broadcast_to(row_coef, (6, K))
    uall[me] = u[...]

    pl.semaphore_wait(barrier, L + T - 2)

    def layer_of(d):
        return lax.rem(me - d + L, L)

    def v_copy(src, c, i, side):
        return remote(src, vline.at[c, i], vs.at[side, c, i], vr.at[c, i], "tensor",
                      right if side == 0 else lft)

    def x_copy(src, slot, dst):
        return remote(src, vall.at[slot], xs.at[dst], xr.at[slot], "layer", dst)

    def u_copy(slot, dst):
        return remote(u, uall.at[slot], us.at[dst], ur.at[slot], "layer", dst)

    def b_copy(slot, dst):
        return remote(cb.at[me], cb.at[slot], bs.at[dst], br.at[slot], "layer", dst)

    def m_copy(slot, dst):
        return remote(mout.at[dst], mi.at[slot], ms.at[dst], mr.at[slot], "layer", dst)

    def l_copy(slot, dst):
        return remote(lall.at[me], lall.at[slot], ls.at[dst], lr.at[slot], "layer", dst)

    def k_copy(slot, dst):
        return remote(core_in.at[t], core_in.at[slot], ks.at[dst], kr.at[slot], "tensor", dst)

    def p_copy(src, d):
        return remote(src, pin.at[d], ps.at[d], pr.at[d], "tensor", right)

    def q_copy(src, d):
        return remote(src, qin.at[d], qs.at[d], qr.at[d], "tensor", lft)

    def piece(i):
        return cols.at[pl.ds(i * PR, PR)]

    for i in range(NP):
        pl.when(has_right)(lambda i=i: v_copy(piece(i), t, i, 0).start())
        pl.when(has_left)(lambda i=i: v_copy(piece(i), t, i, 1).start())

    def send_basis(d):
        dst = lax.rem(me + d, L)
        u_copy(me, dst).start()
        b_copy(me, dst).start()

    loop(1, L, send_basis)

    def spread(c, i, rows):
        def one(b):
            dst = c * B + i * BP + b
            pl.when(dst != me)(lambda: x_copy(rows(b), me, dst).start())

            @pl.when(dst == me)
            def _():
                vall[me] = rows(b)[...]

        loop(0, BP, one)

    for i in range(NP):
        spread(t, i, lambda b, i=i: cols.at[pl.ds(pl.multiple_of(i * PR + b * W, 128), W)])

    @pl.when(t == 0)
    def _():
        loop(0, L, lambda d: pin.__setitem__(d, jnp.zeros(pin.shape[1:], BF16)))

    @pl.when(t == T - 1)
    def _():
        loop(0, L, lambda d: qin.__setitem__(d, jnp.zeros(qin.shape[1:], BF16)))

    def project(d):
        l = layer_of(d)

        @pl.when(d > 0)
        def _():
            u_copy(l, l).wait_recv()
            b_copy(l, l).wait_recv()

        block = g[l]
        own[d] = dot(uall[l], block, ((0,), (0,))).astype(BF16)
        nsend[0, pl.ds(l, 1), :] = lanes(block.astype(F32))

    loop(0, L, project)

    def end_send(d):
        @pl.when((d >= 0) & (d < L))
        def _():
            pl.when(t == 0)(lambda: p_copy(own.at[d], d).start())
            pl.when(t == T - 1)(lambda: q_copy(own.at[d], d).start())

    def forward_p(d):
        @pl.when((d >= 0) & (d < L) & has_left)
        def _():
            p_copy(own.at[d], d).wait_recv()

            @pl.when(has_right)
            def _():
                pin[d] = (pin[d].astype(F32) + own[d].astype(F32)).astype(BF16)
                p_copy(pin.at[d], d).start()

    def forward_q(d):
        @pl.when((d >= 0) & (d < L) & has_right)
        def _():
            q_copy(own.at[d], d).wait_recv()

            @pl.when(has_left)
            def _():
                qin[d] = (qin[d].astype(F32) + own[d].astype(F32)).astype(BF16)
                q_copy(qin.at[d], d).start()

    def relay(h, i):
        for side, c, ok, onward in ((0, t - h, t - h >= 0, has_right), (1, t + h, t + h < T, has_left)):
            @pl.when(ok)
            def _(side=side, c=c, onward=onward):
                v_copy(vline.at[c, i], c, i, side).wait_recv()
                pl.when(onward)(lambda: v_copy(vline.at[c, i], c, i, side).start())
                spread(c, i, lambda b: vline.at[c, i, pl.ds(pl.multiple_of(b * W, 128), W)])

    def middle(d):
        l = layer_of(d)
        pl.when(d > 0)(lambda: x_copy(vall.at[l], l, l).wait_recv())
        m = dot(g[l], vall[l]).astype(BF16)

        @pl.when(d == 0)
        def _():
            mi[me] = m

        @pl.when(d > 0)
        def _():
            mout[l] = m
            m_copy(me, l).start()

    def gather_middle():
        total = mi[me].astype(F32)
        mid[...] = total

        def add(d):
            l = layer_of(d)
            m_copy(l, l).wait_recv()
            mid[...] += mi[l].astype(F32)

        loop(1, L, add)
        core_in[t] = dot(u[...], mid[...].astype(BF16), ((0,), (0,))).astype(BF16)
        loop(1, T, lambda d: k_copy(t, lax.rem(t + d, T)).start())

    def make_left():
        def wait(d):
            s = lax.rem(t + d, T)
            k_copy(s, s).wait_recv()

        loop(1, T, wait)
        core = core_in[0].astype(F32)
        for s in range(1, T):
            core = core + core_in[s].astype(F32)
        core = (core * jnp.transpose(cb[me])[:, 2:3]).astype(BF16)
        mixed = row_base * mid[...] + dot(u[...], core)
        lall[me] = (mixed * dc).astype(BF16)
        loop(1, L, lambda d: l_copy(me, lax.rem(me + d, L)).start())

    sign = jnp.where(inner, -1.0, 1.0).astype(F32)

    def emit(d):
        l = layer_of(d)
        pl.when(d > 0)(lambda: l_copy(l, l).wait_recv())
        total = pin[d].astype(F32) + qin[d].astype(F32) + sign * own[d].astype(F32)
        scaled = (total * jnp.transpose(cb[l])[:, 0:1]).astype(BF16)
        x = cb[l, 1:2, 0:1] * g[l].astype(F32)
        x = x + dot(uall[l], scaled)
        x = x + dot(lall[l], vall[l], ((1,), (1,)))
        raw[l] = x.astype(BF16)
        nsend[1, pl.ds(l, 1), :] = lanes(x)

    blk = lax.div(lax.rem(me, B), BP)
    dist = jnp.abs(t - lax.div(me, B))
    first = jnp.where(dist == 0, 1, NP * (dist - 1) + blk + 1)
    per = max(L // 4, 1)
    at_core = NP * far + 4
    at_left = NP * (T - 1) + 5
    last = max(NP * (T - 1) + L, at_left + 1)

    def emitted(s):
        return jnp.where(s > at_left, jnp.clip(s - NP * far, 0, L), 0)

    def step(s):
        pl.when(s <= NP * (T - 1))(
            lambda: relay(lax.div(s - 1, NP) + 1, lax.rem(s - 1, NP)))
        end_send(s - 1)
        forward_p(s - NP * t - 1)
        forward_q(s - NP * (T - 1 - t) - 1)
        loop(jnp.clip(per * (s - first - 1), 0, L), jnp.clip(per * (s - first), 0, L), middle)
        pl.when(s == at_core)(gather_middle)
        pl.when(s == at_left)(make_left)
        loop(emitted(s - 1), emitted(s), emit)

    loop(1, last + 1, step)

    tile[...] = jnp.zeros_like(tile)
    tile[0:2, 0:L] = jnp.sum(nsend[...], axis=2)

    def n_copy(slot, dst):
        return remote(tile, nin.at[slot], ns.at[dst], nr.at[slot], "tensor", dst)

    loop(1, T, lambda d: n_copy(t, lax.rem(t + d, T)).start())
    nin[t] = tile[...]
    for d in range(1, T):
        s = lax.rem(t + d, T)
        n_copy(s, s).wait_recv()
    sq = nin[0]
    for s in range(1, T):
        sq = sq + nin[s]
    fsend[...] = sq

    def f_copy(slot, dst):
        return remote(fsend, fin.at[slot], fs.at[dst], fr.at[slot], "layer", dst)

    loop(1, L, lambda d: f_copy(me, lax.rem(me + d, L)).start())
    fin[me] = sq

    def finish(d):
        j = lax.rem(me + d, L)
        f_copy(j, j).wait_recv()

    loop(1, L, finish)
    tot = jnp.sum(fin[...], axis=0)
    factor[...] = jnp.broadcast_to(jnp.sqrt((tot[0:1] + 1.0) / (tot[1:2] + 1.0)), factor.shape)

    def drain_layer(d):
        j = lax.rem(me + d, L)
        u_copy(me, j).wait_send()
        b_copy(me, j).wait_send()
        x_copy(vall.at[me], me, j).wait_send()
        m_copy(me, j).wait_send()
        l_copy(me, j).wait_send()
        f_copy(me, j).wait_send()

    loop(1, L, drain_layer)

    def drain_tensor(d):
        s = lax.rem(t + d, T)
        k_copy(t, s).wait_send()
        n_copy(t, s).wait_send()

    loop(1, T, drain_tensor)

    def drain_line(d):
        pl.when(has_right)(lambda: p_copy(own.at[d], d).wait_send())
        pl.when(has_left)(lambda: q_copy(own.at[d], d).wait_send())

    loop(0, L, drain_line)

    def drain_v(c):
        for i in range(NP):
            pl.when((c <= t) & has_right)(lambda i=i: v_copy(piece(i), c, i, 0).wait_send())
            pl.when((c >= t) & has_left)(lambda i=i: v_copy(piece(i), c, i, 1).wait_send())

    loop(0, T, drain_v)


def solution(mesh):
    L, T = mesh.shape["layer"], mesh.shape["tensor"]
    NP = 2

    def body(gradient, row_basis, column_basis, row_eigen, column_eigen, row_escape, column_escape):
        _, r, W = gradient.shape
        _, Cr, K = column_basis.shape
        vmem = pl.BlockSpec(memory_space=pltpu.VMEM)
        chunk = pltpu.VMEM((L, K, W), BF16)
        small = pltpu.VMEM((L, r, K), BF16)
        sem = pltpu.SemaphoreType.DMA
        norms = pltpu.VMEM((8, 128), F32)
        raw, factor = pl.pallas_call(
            functools.partial(kernel, L, T, NP),
            out_shape=(jax.ShapeDtypeStruct((L, r, W), BF16), jax.ShapeDtypeStruct((8, 128), F32)),
            in_specs=[vmem] * 7,
            out_specs=(vmem, vmem),
            scratch_shapes=[
                small,
                pltpu.VMEM((L, W, K), BF16),
                pltpu.VMEM((T, NP, Cr // NP, K), BF16),
                chunk, chunk, chunk,
                small, small,
                pltpu.VMEM((r, K), F32),
                small,
                pltpu.VMEM((T, K, K), BF16),
                pltpu.VMEM((L, 8, K), F32),
                pltpu.VMEM((2, L, 128), F32),
                norms, pltpu.VMEM((T, 8, 128), F32),
                norms, pltpu.VMEM((L, 8, 128), F32),
                sem((L,)), sem((L,)),
                sem((L,)), sem((L,)),
                sem((2, T, NP)), sem((T, NP)),
                sem((L,)), sem((L,)),
                sem((L,)), sem((L,)),
                sem((T,)), sem((T,)),
                sem((L,)), sem((L,)),
                sem((L,)), sem((L,)),
                sem((L,)), sem((L,)),
                sem((T,)), sem((T,)),
                sem((L,)), sem((L,)),
            ],
            compiler_params=pltpu.CompilerParams(
                collective_id=0, has_side_effects=True, vmem_limit_bytes=63 * 1024 * 1024),
        )(gradient, row_basis[0], column_basis[0], row_eigen, column_eigen,
          row_escape[:, None], column_escape[:, None])
        return (raw.astype(F32) * factor[0, :L, None, None]).astype(BF16)

    in_specs = (
        P(None, "tensor", "layer"),
        P("layer", "tensor", None),
        P("layer", "tensor", None),
        P("layer", None),
        P("layer", None),
        P("layer"),
        P("layer"),
    )
    out_specs = P(None, "tensor", "layer")
    return jax.shard_map(body, mesh=mesh, in_specs=in_specs, out_specs=out_specs, check_vma=False)
```

```python
import functools

import jax
import jax.numpy as jnp
from jax import lax
from jax.experimental import pallas as pl
from jax.experimental.pallas import tpu as pltpu
from jax.sharding import PartitionSpec as P

MESH = pl.DeviceIdType.MESH
F32 = jnp.float32
BF16 = jnp.bfloat16


def remote(src, dst, send, recv, axis, index):
    return pltpu.make_async_remote_copy(
        src_ref=src,
        dst_ref=dst,
        send_sem=send,
        recv_sem=recv,
        device_id={axis: index},
        device_id_type=MESH,
    )


def loop(lo, hi, fn):
    def step(i, carry):
        fn(i)
        return carry

    lax.fori_loop(lo, hi, step, 0)


def dot(a, b, dims=((1,), (0,))):
    return lax.dot_general(a, b, (dims, ((), ())), preferred_element_type=F32)


def quarter(x):
    return lax.rsqrt(jnp.sqrt(x))


def lanes(x):
    s = jnp.sum(x * x, axis=0, keepdims=True)
    out = s[:, 0:128]
    for k in range(1, x.shape[1] // 128):
        out = out + s[:, k * 128:(k + 1) * 128]
    return out


def kernel(
    L, T, NP,
    g_hbm, u, cols_hbm, reig, ceig, resc, cesc,
    raw, factor,
    g, uall, vall, vline, own, pin, qin, mout, mi, mid, lall, core_out, core_in, core_sum, cb,
    nsend, tile, nin,
    us, ur, bs, br, vs, vr, xs, xr, ms, mr, ks, kr, ls, lr, ps, pr, qs, qr, ns, nr, gs, cs,
):
    me = lax.axis_index("layer")
    t = lax.axis_index("tensor")
    W = g.shape[2]
    Cr = cols_hbm.shape[0]
    B = Cr // W
    BP = B // NP
    PR = Cr // NP
    K = u.shape[1]
    right, lft = t + 1, t - 1
    has_right, has_left = t < T - 1, t > 0
    inner = has_right & has_left
    far = jnp.maximum(t, T - 1 - t)

    here = me * T + t
    N = L * T

    def g_in(l):
        return pltpu.make_async_copy(g_hbm.at[l], g.at[l], gs.at[l])

    def cols_in(i):
        return pltpu.make_async_copy(cols_hbm.at[pl.ds(i * PR, PR)], vline.at[t, i], cs.at[i])

    for i in range(NP):
        cols_in(i).start()

    def greet(d):
        o = lax.rem(here + d, N)
        pl.semaphore_signal(
            barrier, inc=1, device_id={"layer": lax.div(o, T), "tensor": lax.rem(o, T)}, device_id_type=MESH)

    barrier = pltpu.get_barrier_semaphore()
    loop(1, N, greet)
    loop(0, L, lambda d: g_in(lax.rem(me - d + L, L)).start())

    row_base = quarter(resc[...])
    column_base = quarter(cesc[...])
    row_coef = quarter(reig[...] + resc[...]) - row_base
    dc = quarter(ceig[...] + cesc[...]) - column_base
    cb[me, 0:1, :] = row_coef * column_base
    cb[me, 1:2, :] = jnp.broadcast_to(row_base * column_base, (1, K))
    cb[me, 2:8, :] = jnp.broadcast_to(row_coef, (6, K))
    uall[me] = u[...]

    for i in range(NP):
        cols_in(i).wait()
    pl.semaphore_wait(barrier, N - 1)

    def layer_of(d):
        return lax.rem(me - d + L, L)

    def v_copy(src, c, i, side):
        return remote(src, vline.at[c, i], vs.at[side, c, i], vr.at[c, i], "tensor",
                      right if side == 0 else lft)

    def x_copy(src, slot, dst):
        return remote(src, vall.at[slot], xs.at[dst], xr.at[slot], "layer", dst)

    def u_copy(slot, dst):
        return remote(u, uall.at[slot], us.at[dst], ur.at[slot], "layer", dst)

    def b_copy(slot, dst):
        return remote(cb.at[me], cb.at[slot], bs.at[dst], br.at[slot], "layer", dst)

    def m_copy(slot, dst):
        return remote(mout.at[dst], mi.at[slot], ms.at[dst], mr.at[slot], "layer", dst)

    def l_copy(slot, dst):
        return remote(lall.at[me], lall.at[slot], ls.at[dst], lr.at[slot], "layer", dst)

    def k_copy(src, side):
        return remote(src, core_in.at[side], ks.at[side], kr.at[side], "tensor", right if side == 0 else lft)

    def p_copy(src, d):
        return remote(src, pin.at[d], ps.at[d], pr.at[d], "tensor", right)

    def q_copy(src, d):
        return remote(src, qin.at[d], qs.at[d], qr.at[d], "tensor", lft)

    for i in range(NP):
        pl.when(has_right)(lambda i=i: v_copy(vline.at[t, i], t, i, 0).start())
        pl.when(has_left)(lambda i=i: v_copy(vline.at[t, i], t, i, 1).start())

    def send_basis(d):
        dst = lax.rem(me + d, L)
        u_copy(me, dst).start()
        b_copy(me, dst).start()

    loop(1, L, send_basis)

    def spread(c, i):
        def rows(b):
            return vline.at[c, i, pl.ds(pl.multiple_of(b * W, 128), W)]

        def one(b):
            dst = c * B + i * BP + b
            pl.when(dst != me)(lambda: x_copy(rows(b), me, dst).start())

            @pl.when(dst == me)
            def _():
                vall[me] = rows(b)[...]

        loop(0, BP, one)

    for i in range(NP):
        spread(t, i)

    @pl.when(t == 0)
    def _():
        loop(0, L, lambda d: pin.__setitem__(d, jnp.zeros(pin.shape[1:], BF16)))

    @pl.when(t == T - 1)
    def _():
        loop(0, L, lambda d: qin.__setitem__(d, jnp.zeros(qin.shape[1:], BF16)))

    def project(d):
        l = layer_of(d)

        @pl.when(d > 0)
        def _():
            u_copy(l, l).wait_recv()
            b_copy(l, l).wait_recv()

        g_in(l).wait()
        block = g[l]
        own[d] = dot(uall[l], block, ((0,), (0,))).astype(BF16)
        nsend[0, pl.ds(l, 1), :] = lanes(block.astype(F32))

    loop(0, L, project)

    def end_send(d):
        @pl.when((d >= 0) & (d < L))
        def _():
            pl.when(t == 0)(lambda: p_copy(own.at[d], d).start())
            pl.when(t == T - 1)(lambda: q_copy(own.at[d], d).start())

    def core_pass(side, onward):
        k_copy(core_out, side).wait_recv()

        @pl.when(onward)
        def _():
            core_sum[side] = (core_in[side].astype(F32) + core_out[...].astype(F32)).astype(BF16)
            k_copy(core_sum.at[side], side).start()

    def forward(s, tau, copy, buf, side):
        d = s - NP * tau - 1
        ok = (d >= 0) & (d < L) & inner
        pl.when(ok)(lambda: copy(own.at[0], d).wait_recv())
        pl.when(inner & (s == at_core_end + tau))(lambda: core_pass(side, True))

        @pl.when(ok)
        def _():
            buf[d] = (buf[d].astype(F32) + own[d].astype(F32)).astype(BF16)
            copy(buf.at[d], d).start()

    def relay(h, i):
        for side, c, ok, onward in ((0, t - h, t - h >= 0, has_right), (1, t + h, t + h < T, has_left)):
            @pl.when(ok)
            def _(side=side, c=c, onward=onward):
                v_copy(vline.at[c, i], c, i, side).wait_recv()
                pl.when(onward)(lambda: v_copy(vline.at[c, i], c, i, side).start())
                spread(c, i)

    def middle(d):
        l = layer_of(d)
        pl.when(d > 0)(lambda: x_copy(vall.at[l], l, l).wait_recv())
        m = dot(g[l], vall[l]).astype(BF16)

        @pl.when(d == 0)
        def _():
            mi[me] = m

        @pl.when(d > 0)
        def _():
            mout[l] = m
            m_copy(me, l).start()

    def gather_middle():
        total = mi[me].astype(F32)
        mid[...] = total

        def add(d):
            l = layer_of(d)
            m_copy(l, l).wait_recv()
            mid[...] += mi[l].astype(F32)

        loop(1, L, add)
        core_out[...] = dot(u[...], mid[...].astype(BF16), ((0,), (0,))).astype(BF16)

        @pl.when(t == 0)
        def _():
            core_in[0] = jnp.zeros(core_out.shape, BF16)
            k_copy(core_out, 0).start()

        @pl.when(t == T - 1)
        def _():
            core_in[1] = jnp.zeros(core_out.shape, BF16)
            k_copy(core_out, 1).start()

    def make_left():
        pl.when(t == 0)(lambda: core_pass(1, False))
        pl.when(t == T - 1)(lambda: core_pass(0, False))
        core = core_in[0].astype(F32) + core_in[1].astype(F32) + core_out[...].astype(F32)
        core = (core * jnp.transpose(cb[me])[:, 2:3]).astype(BF16)
        mixed = row_base * mid[...] + dot(u[...], core)
        lall[me] = (mixed * dc).astype(BF16)
        loop(1, L, lambda d: l_copy(me, lax.rem(me + d, L)).start())

    sign = jnp.where(inner, -1.0, 1.0).astype(F32)

    def emit(d):
        l = layer_of(d)
        pl.when(d > 0)(lambda: l_copy(l, l).wait_recv())
        pl.when(t == T - 1)(lambda: p_copy(own.at[d], d).wait_recv())
        pl.when(t == 0)(lambda: q_copy(own.at[d], d).wait_recv())
        total = pin[d].astype(F32) + qin[d].astype(F32) + sign * own[d].astype(F32)
        scaled = (total * jnp.transpose(cb[l])[:, 0:1]).astype(BF16)
        x = cb[l, 1:2, 0:1] * g[l].astype(F32)
        x = x + dot(uall[l], scaled)
        x = x + dot(lall[l], vall[l], ((1,), (1,)))
        raw[l] = x.astype(BF16)
        nsend[1, pl.ds(l, 1), :] = lanes(x)

    blk = lax.div(lax.rem(me, B), BP)
    dist = jnp.abs(t - lax.div(me, B))
    first = jnp.where(dist == 0, 1, NP * (dist - 1) + blk + 1)
    per = max(L // 4, 1)
    at_core = NP * far + 4
    at_core_end = NP * (T - 1) + 3
    last = max(NP * (T - 2) + L, at_core_end + T - 2, NP * (T - 1) + 4)

    def step(s):
        pl.when(s <= NP * (T - 1))(
            lambda: relay(lax.div(s - 1, NP) + 1, lax.rem(s - 1, NP)))
        end_send(s - 1)
        forward(s, t, p_copy, pin, 0)
        forward(s, T - 1 - t, q_copy, qin, 1)
        loop(jnp.clip(per * (s - first - 1), 0, L), jnp.clip(per * (s - first), 0, L), middle)
        pl.when(s == at_core)(gather_middle)

    loop(1, last + 1, step)
    make_left()
    loop(0, L, emit)

    tile[...] = jnp.zeros_like(tile)
    tile[0:2, 0:L] = jnp.sum(nsend[...], axis=2)

    def n_copy(slot, dst):
        return pltpu.make_async_remote_copy(
            src_ref=tile, dst_ref=nin.at[slot], send_sem=ns.at[dst], recv_sem=nr.at[slot],
            device_id={"layer": lax.div(dst, T), "tensor": lax.rem(dst, T)}, device_id_type=MESH)

    loop(1, N, lambda d: n_copy(here, lax.rem(here + d, N)).start())
    nin[here] = tile[...]

    def finish(d):
        o = lax.rem(here + d, N)
        n_copy(o, o).wait_recv()

    loop(1, N, finish)
    tot = jnp.sum(nin[...], axis=0)
    fac = jnp.broadcast_to(jnp.sqrt((tot[0:1] + 1.0) / (tot[1:2] + 1.0)), (8, 128))
    factor[...] = jnp.broadcast_to(jnp.transpose(fac)[0:L, 0:1], factor.shape)

    def drain_layer(d):
        j = lax.rem(me + d, L)
        u_copy(me, j).wait_send()
        b_copy(me, j).wait_send()
        x_copy(vall.at[me], me, j).wait_send()
        m_copy(me, j).wait_send()
        l_copy(me, j).wait_send()

    loop(1, L, drain_layer)

    pl.when(has_right)(lambda: k_copy(core_out, 0).wait_send())
    pl.when(has_left)(lambda: k_copy(core_out, 1).wait_send())

    def drain_norm(d):
        o = lax.rem(here + d, N)
        n_copy(here, o).wait_send()

    loop(1, N, drain_norm)

    def drain_line(d):
        pl.when(has_right)(lambda: p_copy(own.at[d], d).wait_send())
        pl.when(has_left)(lambda: q_copy(own.at[d], d).wait_send())

    loop(0, L, drain_line)

    def drain_v(c):
        for i in range(NP):
            pl.when((c <= t) & has_right)(lambda i=i: v_copy(vline.at[c, i], c, i, 0).wait_send())
            pl.when((c >= t) & has_left)(lambda i=i: v_copy(vline.at[c, i], c, i, 1).wait_send())

    loop(0, T, drain_v)


def scale_kernel(raw, factor, out, buf, sem):
    def one(l):
        buf[l] = (raw[l].astype(F32) * factor[pl.ds(l, 1), 0:1]).astype(BF16)
        pltpu.make_async_copy(buf.at[l], out.at[l], sem.at[l]).start()

    L = raw.shape[0]
    loop(0, L, one)
    loop(0, L, lambda l: pltpu.make_async_copy(buf.at[l], out.at[l], sem.at[l]).wait())


def solution(mesh):
    L, T = mesh.shape["layer"], mesh.shape["tensor"]
    NP = 2

    def body(gradient, row_basis, column_basis, row_eigen, column_eigen, row_escape, column_escape):
        _, r, W = gradient.shape
        _, Cr, K = column_basis.shape
        vmem = pl.BlockSpec(memory_space=pltpu.VMEM)
        hbm = pl.BlockSpec(memory_space=pl.ANY)
        chunk = pltpu.VMEM((L, K, W), BF16)
        small = pltpu.VMEM((L, r, K), BF16)
        sem = pltpu.SemaphoreType.DMA
        raw, factor = pl.pallas_call(
            functools.partial(kernel, L, T, NP),
            out_shape=(pltpu.VMEM((L, r, W), BF16), pltpu.VMEM((L, 128), F32)),
            in_specs=[hbm, vmem, hbm, vmem, vmem, vmem, vmem],
            out_specs=(vmem, vmem),
            scratch_shapes=[
                pltpu.VMEM((L, r, W), BF16),
                small,
                pltpu.VMEM((L, W, K), BF16),
                pltpu.VMEM((T, NP, Cr // NP, K), BF16),
                chunk, chunk, chunk,
                small, small,
                pltpu.VMEM((r, K), F32),
                small,
                pltpu.VMEM((K, K), BF16),
                pltpu.VMEM((2, K, K), BF16),
                pltpu.VMEM((2, K, K), BF16),
                pltpu.VMEM((L, 8, K), F32),
                pltpu.VMEM((2, L, 128), F32),
                pltpu.VMEM((8, 128), F32),
                pltpu.VMEM((L * T, 8, 128), F32),
                sem((L,)), sem((L,)),
                sem((L,)), sem((L,)),
                sem((2, T, NP)), sem((T, NP)),
                sem((L,)), sem((L,)),
                sem((L,)), sem((L,)),
                sem((2,)), sem((2,)),
                sem((L,)), sem((L,)),
                sem((L,)), sem((L,)),
                sem((L,)), sem((L,)),
                sem((L * T,)), sem((L * T,)),
                sem((L,)), sem((NP,)),
            ],
            compiler_params=pltpu.CompilerParams(
                collective_id=0, has_side_effects=True, vmem_limit_bytes=67043328 - 2 * L * r * W - 256 * 1024),
        )(gradient, row_basis[0], column_basis[0], row_eigen, column_eigen,
          row_escape[:, None], column_escape[:, None])
        return pl.pallas_call(
            scale_kernel,
            out_shape=jax.ShapeDtypeStruct((L, r, W), BF16),
            in_specs=[vmem, vmem],
            out_specs=hbm,
            scratch_shapes=[pltpu.VMEM((L, r, W), BF16), sem((L,))],
            compiler_params=pltpu.CompilerParams(vmem_limit_bytes=32 * 1024 * 1024),
        )(raw, factor)

    in_specs = (
        P(None, "tensor", "layer"),
        P("layer", "tensor", None),
        P("layer", "tensor", None),
        P("layer", None),
        P("layer", None),
        P("layer"),
        P("layer"),
    )
    out_specs = P(None, "tensor", "layer")
    return jax.shard_map(body, mesh=mesh, in_specs=in_specs, out_specs=out_specs, check_vma=False)
```

```python
import functools

import jax
import jax.numpy as jnp
from jax import lax
from jax.experimental import pallas as pl
from jax.experimental.pallas import tpu as pltpu
from jax.sharding import PartitionSpec as P

MESH = pl.DeviceIdType.MESH
F32 = jnp.float32
BF16 = jnp.bfloat16


def remote(src, dst, send, recv, axis, index):
    return pltpu.make_async_remote_copy(
        src_ref=src,
        dst_ref=dst,
        send_sem=send,
        recv_sem=recv,
        device_id={axis: index},
        device_id_type=MESH,
    )


def loop(lo, hi, fn):
    def step(i, carry):
        fn(i)
        return carry

    lax.fori_loop(lo, hi, step, 0)


def dot(a, b, dims=((1,), (0,))):
    return lax.dot_general(a, b, (dims, ((), ())), preferred_element_type=F32)


def quarter(x):
    return lax.rsqrt(jnp.sqrt(x))


def lanes(x):
    s = jnp.sum(x * x, axis=0, keepdims=True)
    out = s[:, 0:128]
    for k in range(1, x.shape[1] // 128):
        out = out + s[:, k * 128:(k + 1) * 128]
    return out


def kernel(
    L, T, NP,
    g_hbm, u, cols_hbm, reig, ceig, resc, cesc,
    raw, factor,
    g, uall, vall, vline, own, pin, qin, mout, mi, mid, lall, core_out, core_in, core_sum, cb,
    guest_g, guest_u, guest_l, guest_x, guest_n, nsend, tile, nin,
    us, ur, bs, br, vs, vr, xs, xr, ms, mr, ks, kr, ls, lr, ps, pr, qs, qr, ns, nr, hs, hr, gs, cs,
):
    me = lax.axis_index("layer")
    t = lax.axis_index("tensor")
    W = g.shape[2]
    K = u.shape[1]
    right, lft = t + 1, t - 1
    has_right, has_left = t < T - 1, t > 0
    inner = has_right & has_left
    far = jnp.maximum(t, T - 1 - t)
    n_left, n_right = t, T - 1 - t

    here = me * T + t
    N = L * T

    def g_in(l):
        return pltpu.make_async_copy(g_hbm.at[l], g.at[l], gs.at[l])

    def cols_in(i):
        return pltpu.make_async_copy(cols_hbm.at[pl.ds(i * W, W)], vline.at[t, i], cs.at[i])

    for i in range(NP):
        cols_in(i).start()

    def greet(d):
        o = lax.rem(here + d, N)
        pl.semaphore_signal(
            barrier, inc=1, device_id={"layer": lax.div(o, T), "tensor": lax.rem(o, T)}, device_id_type=MESH)

    barrier = pltpu.get_barrier_semaphore()
    loop(1, N, greet)
    loop(0, L, lambda d: g_in(lax.rem(me + d, L)).start())

    tile[...] = jnp.zeros_like(tile)
    row_base = quarter(resc[...])
    column_base = quarter(cesc[...])
    row_coef = quarter(reig[...] + resc[...]) - row_base
    dc = quarter(ceig[...] + cesc[...]) - column_base
    cb[me, 0:1, :] = row_coef * column_base
    cb[me, 1:2, :] = jnp.broadcast_to(row_base * column_base, (1, K))
    cb[me, 2:8, :] = jnp.broadcast_to(row_coef, (6, K))
    uall[me] = u[...]

    for i in range(NP):
        cols_in(i).wait()
    pl.semaphore_wait(barrier, N - 1)

    def layer_of(d):
        return lax.rem(me + d, L)

    def v_copy(src, c, i, side):
        return remote(src, vline.at[c, i], vs.at[side, c, i], vr.at[c, i], "tensor",
                      right if side == 0 else lft)

    def x_copy(src, slot, dst):
        return remote(src, vall.at[slot], xs.at[dst], xr.at[slot], "layer", dst)

    def u_copy(slot, dst):
        return remote(u, uall.at[slot], us.at[dst], ur.at[slot], "layer", dst)

    def b_copy(slot, dst):
        return remote(cb.at[me], cb.at[slot], bs.at[dst], br.at[slot], "layer", dst)

    def m_copy(slot, dst):
        return remote(mout.at[dst], mi.at[slot], ms.at[dst], mr.at[slot], "layer", dst)

    def l_copy(slot, dst):
        return remote(lall.at[me], lall.at[slot], ls.at[dst], lr.at[slot], "layer", dst)

    def k_copy(src, side):
        return remote(src, core_in.at[side], ks.at[side], kr.at[side], "tensor", right if side == 0 else lft)

    def p_copy(src, d):
        return remote(src, pin.at[d], ps.at[d], pr.at[d], "tensor", right)

    def q_copy(src, d):
        return remote(src, qin.at[d], qs.at[d], qr.at[d], "tensor", lft)

    def send_own(i, side):
        v_copy(vline.at[t, i], t, i, side).start()

    pl.when(has_right)(lambda: loop(0, jnp.where(has_left, 1, NP), lambda i: send_own(i, 0)))
    pl.when(has_left)(lambda: loop(0, jnp.where(has_right, 1, NP), lambda i: send_own(i, 1)))

    def send_basis(d):
        dst = lax.rem(me - d + L, L)
        u_copy(me, dst).start()
        b_copy(me, dst).start()

    loop(1, L, send_basis)

    def spread(c, i):
        dst = c * NP + i
        pl.when(dst != me)(lambda: x_copy(vline.at[c, i], me, dst).start())

        @pl.when(dst == me)
        def _():
            vall[me] = vline[c, i]

    loop(0, NP, lambda i: spread(t, i))

    @pl.when(t == 0)
    def _():
        loop(0, L, lambda d: pin.__setitem__(d, jnp.zeros(pin.shape[1:], BF16)))

    @pl.when(t == T - 1)
    def _():
        loop(0, L, lambda d: qin.__setitem__(d, jnp.zeros(qin.shape[1:], BF16)))

    def project(d):
        l = layer_of(d)

        @pl.when(d > 0)
        def _():
            u_copy(l, l).wait_recv()
            b_copy(l, l).wait_recv()

        g_in(l).wait()
        block = g[l]
        own[d] = dot(uall[l], block, ((0,), (0,))).astype(BF16)
        nsend[0, pl.ds(l, 1), :] = lanes(block.astype(F32))

    loop(0, L, project)

    def end_send(d):
        @pl.when((d >= 0) & (d < L))
        def _():
            pl.when(t == 0)(lambda: p_copy(own.at[d], d).start())
            pl.when(t == T - 1)(lambda: q_copy(own.at[d], d).start())

    def core_pass(side, onward):
        k_copy(core_out, side).wait_recv()

        @pl.when(onward)
        def _():
            core_sum[side] = (core_in[side].astype(F32) + core_out[...].astype(F32)).astype(BF16)
            k_copy(core_sum.at[side], side).start()

    def forward(s, tau, copy, buf, side):
        d = s - NP * tau - 1
        ok = (d >= 0) & (d < L) & inner
        pl.when(ok)(lambda: copy(own.at[0], d).wait_recv())
        pl.when(inner & (s == at_core_end + tau))(lambda: core_pass(side, True))

        @pl.when(ok)
        def _():
            buf[d] = (buf[d].astype(F32) + own[d].astype(F32)).astype(BF16)
            pl.when((d < L - 1) | (tau < T - 2))(lambda: copy(buf.at[d], d).start())

    def relay(s, n, way, side, onward):
        near = jnp.maximum(n, 1)
        i, h = lax.div(s - 1, near), lax.rem(s - 1, near) + 1
        c = t + way * h

        @pl.when(s <= NP * n)
        def _():
            v_copy(vline.at[c, i], c, i, side).wait_recv()
            pl.when(onward)(lambda: v_copy(vline.at[c, i], c, i, side).start())
            pl.when(onward & (h == n) & (i + 1 < NP))(lambda: send_own(i + 1, side))
            spread(c, i)

    def middle(d):
        l = layer_of(d)
        pl.when(d > 0)(lambda: x_copy(vall.at[l], l, l).wait_recv())
        m = dot(g[l], vall[l]).astype(BF16)

        @pl.when(d == 0)
        def _():
            mi[me] = m

        @pl.when(d > 0)
        def _():
            mout[l] = m
            m_copy(me, l).start()

    def gather_middle():
        total = mi[me].astype(F32)
        mid[...] = total

        def add(d):
            l = layer_of(d)
            m_copy(l, l).wait_recv()
            mid[...] += mi[l].astype(F32)

        loop(1, L, add)
        core_out[...] = dot(u[...], mid[...].astype(BF16), ((0,), (0,))).astype(BF16)

        @pl.when(t == 0)
        def _():
            core_in[0] = jnp.zeros(core_out.shape, BF16)
            k_copy(core_out, 0).start()

        @pl.when(t == T - 1)
        def _():
            core_in[1] = jnp.zeros(core_out.shape, BF16)
            k_copy(core_out, 1).start()

    def make_left():
        core = core_in[0].astype(F32) + core_in[1].astype(F32) + core_out[...].astype(F32)
        core = (core * jnp.transpose(cb[me])[:, 2:3]).astype(BF16)
        mixed = row_base * mid[...] + dot(u[...], core)
        lall[me] = (mixed * dc).astype(BF16)
        loop(1, L, lambda d: l_copy(me, lax.rem(me + d, L)).start())

    sign = jnp.where(inner, -1.0, 1.0).astype(F32)

    def pushed(d):
        total = pin[d].astype(F32) + qin[d].astype(F32) + sign * own[d].astype(F32)
        return (total * jnp.transpose(cb[layer_of(d)])[:, 0:1]).astype(BF16)

    def update(l, block, basis, scaled, left):
        x = cb[l, 1:2, 0:1] * block.astype(F32)
        x = x + dot(basis, scaled)
        return x + dot(left, vall[l], ((1,), (1,)))

    def emit(d):
        l = layer_of(d)
        pl.when(d > 0)(lambda: l_copy(l, l).wait_recv())
        pl.when(t == T - 1)(lambda: p_copy(own.at[d], d).wait_recv())
        pl.when(t == 0)(lambda: q_copy(own.at[d], d).wait_recv())
        x = update(l, g[l], uall[l], pushed(d), lall[l])
        raw[l] = x.astype(BF16)
        nsend[1, pl.ds(l, 1), :] = lanes(x)

    final = L - 1
    lf = layer_of(final)

    def h_copies(side):
        to = lax.rem(t + (1 if side == 0 else T - 1), T)
        return [
            remote(src, dst, hs.at[k], hr.at[k], "tensor", to)
            for k, (src, dst) in enumerate(((g.at[lf], guest_g), (uall.at[lf], guest_u), (lall.at[lf], guest_l)))]

    def guest_emit():
        for copy in h_copies(0):
            copy.wait_recv()
        x = update(lf, guest_g[...], guest_u[...], pushed(final), guest_l[...])
        guest_x[...] = x.astype(BF16)
        guest_n[...] = lanes(x)
        pl.when(t == T - 2)(lambda: p_copy(guest_x, final).start())
        pl.when(t == 1)(lambda: q_copy(guest_x, final).start())

    blk = lax.rem(me, NP)
    home = lax.div(me, NP)
    dist = jnp.abs(t - home)
    first = jnp.where(dist == 0, 2 * blk + 3, blk * jnp.where(home < t, n_left, n_right) + dist + 2)
    at_core = NP * far + 2
    at_core_end = NP * (T - 1) + 2
    last = max(NP * (T - 2) + L, at_core_end + T - 2, NP * (T - 1) + 2, 2 * NP + 1)

    def step(s):
        relay(s, n_left, -1, 0, has_right)
        relay(s, n_right, 1, 1, has_left)
        pl.when(s < L)(lambda: end_send(s - 1))
        forward(s, t, p_copy, pin, 0)
        forward(s, T - 1 - t, q_copy, qin, 1)
        loop(jnp.where(s == first, 0, L), L, middle)

        @pl.when(s == at_core)
        def _():
            gather_middle()
            end_send(L - 1)

        pl.when(inner & (s == at_core_end + T - 2))(make_left)

    guest_n[...] = jnp.zeros_like(guest_n)
    nsend[1, pl.ds(lf, 1), :] = jnp.zeros((1, 128), F32)
    loop(1, last + 1, step)

    def end_left(side):
        copies = h_copies(side)
        copies[0].start()
        copies[1].start()
        core_pass(1 - side, False)
        make_left()
        l_copy(lf, lf).wait_recv()
        copies[2].start()

    pl.when(t == 0)(lambda: end_left(0))
    pl.when(t == T - 1)(lambda: end_left(1))
    pl.when((t == 1) | (t == T - 2))(guest_emit)
    loop(0, jnp.where(inner, L, L - 1), emit)

    nsend[1, pl.ds(lf, 1), :] = nsend[1, pl.ds(lf, 1), :] + guest_n[...]
    sums = jnp.sum(nsend[...], axis=2)
    tile[0:1, 0:L] = sums[0:1]
    tile[0:1, L:2 * L] = sums[1:2]

    def n_copy(slot, dst):
        return pltpu.make_async_remote_copy(
            src_ref=tile, dst_ref=nin.at[slot], send_sem=ns.at[dst], recv_sem=nr.at[slot],
            device_id={"layer": lax.div(dst, T), "tensor": lax.rem(dst, T)}, device_id_type=MESH)

    loop(1, N, lambda d: n_copy(here, lax.rem(here + d, N)).start())
    nin[here] = tile[...]

    def drain_layer(d):
        j = lax.rem(me + d, L)
        u_copy(me, j).wait_send()
        b_copy(me, j).wait_send()
        x_copy(vall.at[me], me, j).wait_send()
        m_copy(me, j).wait_send()
        l_copy(me, j).wait_send()

    loop(1, L, drain_layer)

    pl.when(has_right)(lambda: k_copy(core_out, 0).wait_send())
    pl.when(has_left)(lambda: k_copy(core_out, 1).wait_send())

    def drain_line(d):
        pl.when(has_right)(lambda: p_copy(own.at[d], d).wait_send())
        pl.when(has_left)(lambda: q_copy(own.at[d], d).wait_send())

    loop(0, L, drain_line)

    def drain_v(c):
        for i in range(NP):
            pl.when((c <= t) & has_right)(lambda i=i: v_copy(vline.at[c, i], c, i, 0).wait_send())
            pl.when((c >= t) & has_left)(lambda i=i: v_copy(vline.at[c, i], c, i, 1).wait_send())

    loop(0, T, drain_v)

    for side, end in ((0, 0), (1, T - 1)):
        @pl.when(t == end)
        def _(side=side):
            for copy in h_copies(side):
                copy.wait_send()

    def finish(d):
        o = lax.rem(here + d, N)
        n_copy(o, o).wait_recv()

    loop(1, N, finish)
    tot = jnp.sum(nin[...], axis=0)
    fac = jnp.sqrt((tot[:, 0:L] + 1.0) / (tot[:, L:2 * L] + 1.0))
    factor[...] = jnp.broadcast_to(jnp.transpose(jnp.broadcast_to(fac, (8, L)))[:, 0:1], factor.shape)

    def drain_norm(d):
        o = lax.rem(here + d, N)
        n_copy(here, o).wait_send()

    loop(1, N, drain_norm)

    @pl.when(t == T - 1)
    def _():
        p_copy(own.at[final], final).wait_recv()
        raw[lf] = pin[final]

    @pl.when(t == 0)
    def _():
        q_copy(own.at[final], final).wait_recv()
        raw[lf] = qin[final]


def scale_kernel(raw, factor, out, buf, sem):
    def one(l):
        buf[l] = (raw[l].astype(F32) * factor[pl.ds(l, 1), 0:1]).astype(BF16)
        pltpu.make_async_copy(buf.at[l], out.at[l], sem.at[l]).start()

    L = raw.shape[0]
    loop(0, L, one)
    loop(0, L, lambda l: pltpu.make_async_copy(buf.at[l], out.at[l], sem.at[l]).wait())


def solution(mesh):
    L, T = mesh.shape["layer"], mesh.shape["tensor"]
    NP = L // T

    def body(gradient, row_basis, column_basis, row_eigen, column_eigen, row_escape, column_escape):
        _, r, W = gradient.shape
        _, Cr, K = column_basis.shape
        vmem = pl.BlockSpec(memory_space=pltpu.VMEM)
        hbm = pl.BlockSpec(memory_space=pl.ANY)
        chunk = pltpu.VMEM((L, K, W), BF16)
        small = pltpu.VMEM((L, r, K), BF16)
        sem = pltpu.SemaphoreType.DMA
        raw, factor = pl.pallas_call(
            functools.partial(kernel, L, T, NP),
            out_shape=(pltpu.VMEM((L, r, W), BF16), pltpu.VMEM((L, 128), F32)),
            in_specs=[hbm, vmem, hbm, vmem, vmem, vmem, vmem],
            out_specs=(vmem, vmem),
            scratch_shapes=[
                pltpu.VMEM((L, r, W), BF16),
                small,
                pltpu.VMEM((L, W, K), BF16),
                pltpu.VMEM((T, NP, Cr // NP, K), BF16),
                chunk, chunk, chunk,
                small, small,
                pltpu.VMEM((r, K), F32),
                small,
                pltpu.VMEM((K, K), BF16),
                pltpu.VMEM((2, K, K), BF16),
                pltpu.VMEM((2, K, K), BF16),
                pltpu.VMEM((L, 8, K), F32),
                pltpu.VMEM((r, W), BF16),
                pltpu.VMEM((r, K), BF16),
                pltpu.VMEM((r, K), BF16),
                pltpu.VMEM((r, W), BF16),
                pltpu.VMEM((1, 128), F32),
                pltpu.VMEM((2, L, 128), F32),
                pltpu.VMEM((1, 128), F32),
                pltpu.VMEM((L * T, 1, 128), F32),
                sem((L,)), sem((L,)),
                sem((L,)), sem((L,)),
                sem((2, T, NP)), sem((T, NP)),
                sem((L,)), sem((L,)),
                sem((L,)), sem((L,)),
                sem((2,)), sem((2,)),
                sem((L,)), sem((L,)),
                sem((L,)), sem((L,)),
                sem((L,)), sem((L,)),
                sem((L * T,)), sem((L * T,)),
                sem((3,)), sem((3,)),
                sem((L,)), sem((NP,)),
            ],
            compiler_params=pltpu.CompilerParams(
                collective_id=0, has_side_effects=True, vmem_limit_bytes=67043328 - 2 * L * r * W - 256 * 1024),
        )(gradient, row_basis[0], column_basis[0], row_eigen, column_eigen,
          row_escape[:, None], column_escape[:, None])
        return pl.pallas_call(
            scale_kernel,
            out_shape=jax.ShapeDtypeStruct((L, r, W), BF16),
            in_specs=[vmem, vmem],
            out_specs=hbm,
            scratch_shapes=[pltpu.VMEM((L, r, W), BF16), sem((L,))],
            compiler_params=pltpu.CompilerParams(vmem_limit_bytes=32 * 1024 * 1024),
        )(raw, factor)

    in_specs = (
        P(None, "tensor", "layer"),
        P("layer", "tensor", None),
        P("layer", "tensor", None),
        P("layer", None),
        P("layer", None),
        P("layer"),
        P("layer"),
    )
    out_specs = P(None, "tensor", "layer")
    return jax.shard_map(body, mesh=mesh, in_specs=in_specs, out_specs=out_specs, check_vma=False)
```

```python
import functools

import jax
import jax.numpy as jnp
from jax import lax
from jax.experimental import pallas as pl
from jax.experimental.pallas import tpu as pltpu
from jax.sharding import PartitionSpec as P

MESH = pl.DeviceIdType.MESH
F32 = jnp.float32
BF16 = jnp.bfloat16


def remote(src, dst, send, recv, axis, index):
    return pltpu.make_async_remote_copy(
        src_ref=src,
        dst_ref=dst,
        send_sem=send,
        recv_sem=recv,
        device_id={axis: index},
        device_id_type=MESH,
    )


def loop(lo, hi, fn):
    def step(i, carry):
        fn(i)
        return carry

    lax.fori_loop(lo, hi, step, 0)


def dot(a, b, dims=((1,), (0,))):
    return lax.dot_general(a, b, (dims, ((), ())), preferred_element_type=F32)


def quarter(x):
    return lax.rsqrt(jnp.sqrt(x))


def lanes(x):
    s = jnp.sum(x * x, axis=0, keepdims=True)
    out = s[:, 0:128]
    for k in range(1, x.shape[1] // 128):
        out = out + s[:, k * 128:(k + 1) * 128]
    return out


def kernel(
    L, T, NP,
    g_hbm, u, cols_hbm, reig, ceig, resc, cesc,
    raw, factor,
    g, uall, vall, vline, own, pin, qin, mout, mi, mid, lall, core_out, core_in, core_sum, cb,
    guest_g, guest_u, guest_l, guest_x, guest_n, nsend, tile, nin,
    us, ur, bs, br, vs, vr, xs, xr, ms, mr, ks, kr, ls, lr, ps, pr, qs, qr, ns, nr, hs, hr, gs, cs,
):
    me = lax.axis_index("layer")
    t = lax.axis_index("tensor")
    W = g.shape[2]
    K = u.shape[1]
    right, lft = t + 1, t - 1
    has_right, has_left = t < T - 1, t > 0
    inner = has_right & has_left
    far = jnp.maximum(t, T - 1 - t)
    n_left, n_right = t, T - 1 - t

    here = me * T + t
    N = L * T

    g_in = pltpu.make_async_copy(g_hbm, g, gs)

    def cols_in(i):
        return pltpu.make_async_copy(cols_hbm.at[pl.ds(i * W, W)], vline.at[t, i], cs.at[i])

    for i in range(NP):
        cols_in(i).start()

    def greet(axis, index):
        pl.semaphore_signal(barrier, inc=1, device_id={axis: index}, device_id_type=MESH)

    barrier = pltpu.get_barrier_semaphore()
    pl.when(has_right)(lambda: greet("tensor", right))
    pl.when(has_left)(lambda: greet("tensor", lft))
    loop(1, L, lambda d: greet("layer", lax.rem(me + d, L)))
    g_in.start()

    tile[...] = jnp.zeros_like(tile)
    row_base = quarter(resc[...])
    column_base = quarter(cesc[...])
    row_coef = quarter(reig[...] + resc[...]) - row_base
    dc = quarter(ceig[...] + cesc[...]) - column_base
    cb[me, 0:1, :] = row_coef * column_base
    cb[me, 1:2, :] = jnp.broadcast_to(row_base * column_base, (1, K))
    cb[me, 2:8, :] = jnp.broadcast_to(row_coef, (6, K))
    uall[me] = u[...]

    for i in range(NP):
        cols_in(i).wait()
    pl.semaphore_wait(barrier, L - 1 + jnp.where(inner, 2, 1))

    def layer_of(d):
        return lax.rem(me + d, L)

    def v_copy(src, c, i, side):
        return remote(src, vline.at[c, i], vs.at[side, c], vr.at[c, i], "tensor",
                      right if side == 0 else lft)

    def x_copy(src, slot, dst):
        return remote(src, vall.at[slot], xs, xr.at[slot], "layer", dst)

    def u_copy(slot, dst):
        return remote(u, uall.at[slot], us, ur.at[slot], "layer", dst)

    def b_copy(slot, dst):
        return remote(cb.at[me], cb.at[slot], bs, br.at[slot], "layer", dst)

    def m_copy(slot, dst):
        return remote(mout.at[dst], mi.at[slot], ms, mr, "layer", dst)

    def l_copy(slot, dst):
        return remote(lall.at[me], lall.at[slot], ls, lr.at[slot], "layer", dst)

    def k_copy(src, side):
        return remote(src, core_in.at[side], ks.at[side], kr.at[side], "tensor", right if side == 0 else lft)

    def p_copy(src, d):
        return remote(src, pin.at[d], ps, pr.at[d], "tensor", right)

    def q_copy(src, d):
        return remote(src, qin.at[d], qs, qr.at[d], "tensor", lft)

    def send_own(i, side):
        v_copy(vline.at[t, i], t, i, side).start()

    def send_half(i, half, side):
        rows = vline.at[t, i, pl.ds(half * (W // 2), W // 2)]
        remote(rows, rows, vs.at[side, t], vr.at[t, i], "tensor", right if side == 0 else lft).start()

    def send_first(side, onward, n):
        @pl.when(onward)
        def _():
            loop(0, jnp.where(n > 0, 1, NP), lambda i: send_own(i, side))
            pl.when((n > 0) & (NP > 1))(lambda: send_half(1, 0, side))

    send_first(0, has_right, n_left)
    send_first(1, has_left, n_right)

    def send_basis(d):
        dst = lax.rem(me - d + L, L)
        u_copy(me, dst).start()
        b_copy(me, dst).start()

    loop(1, L, send_basis)

    def spread(c, i):
        dst = c * NP + i
        pl.when(dst != me)(lambda: x_copy(vline.at[c, i], me, dst).start())

        @pl.when(dst == me)
        def _():
            vall[me] = vline[c, i]

    @pl.when(t == 0)
    def _():
        loop(0, L, lambda d: pin.__setitem__(d, jnp.zeros(pin.shape[1:], BF16)))

    @pl.when(t == T - 1)
    def _():
        loop(0, L, lambda d: qin.__setitem__(d, jnp.zeros(qin.shape[1:], BF16)))

    def project(d):
        l = layer_of(d)

        @pl.when(d > 0)
        def _():
            u_copy(l, l).wait_recv()
            b_copy(l, l).wait_recv()

        block = g[l]
        own[d] = dot(uall[l], block, ((0,), (0,))).astype(BF16)
        nsend[0, pl.ds(l, 1), :] = lanes(block.astype(F32))

    g_in.wait()
    project(0)

    def end_send(d):
        @pl.when((d >= 0) & (d < L))
        def _():
            pl.when(t == 0)(lambda: p_copy(own.at[d], d).start())
            pl.when(t == T - 1)(lambda: q_copy(own.at[d], d).start())

    def core_pass(side, onward):
        k_copy(core_out, side).wait_recv()

        @pl.when(onward)
        def _():
            core_sum[side] = (core_in[side].astype(F32) + core_out[...].astype(F32)).astype(BF16)
            k_copy(core_sum.at[side], side).start()

    def forward(s, tau, copy, buf, side):
        d = s - NP * tau - 1
        ok = (d >= 0) & (d < L) & inner
        pl.when(ok)(lambda: copy(own.at[0], d).wait_recv())
        pl.when(inner & (s == at_core_end + tau))(lambda: core_pass(side, True))

        @pl.when(ok)
        def _():
            buf[d] = (buf[d].astype(F32) + own[d].astype(F32)).astype(BF16)
            pl.when((d < L - 1) | (tau < T - 2))(lambda: copy(buf.at[d], d).start())

    def relay(s, n, way, side, onward):
        near = jnp.maximum(n, 1)
        i, h = lax.div(s - 1, near), lax.rem(s - 1, near) + 1
        c = t + way * h

        @pl.when(s <= NP * n)
        def _():
            v_copy(vline.at[c, i], c, i, side).wait_recv()
            pl.when(onward)(lambda: v_copy(vline.at[c, i], c, i, side).start())
            pl.when(onward & (h == 1) & (i + 1 < NP))(lambda: send_half(i + 1, 1, side))
            pl.when(onward & (h == n) & (i + 2 < NP))(lambda: send_half(i + 2, 0, side))
            spread(c, i)

    def middle(d):
        l = layer_of(d)
        pl.when(d > 0)(lambda: x_copy(vall.at[l], l, l).wait_recv())
        m = dot(g[l], vall[l]).astype(BF16)

        @pl.when(d == 0)
        def _():
            mi[me] = m

        @pl.when(d > 0)
        def _():
            mout[l] = m
            m_copy(me, l).start()

    def gather_middle():
        total = mi[me].astype(F32)
        mid[...] = total

        remote(mout.at[pl.ds(0, L - 1)], mi.at[pl.ds(0, L - 1)], ms, mr, "layer", me).wait_recv()

        def add(d):
            mid[...] += mi[layer_of(d)].astype(F32)

        loop(1, L, add)
        core_out[...] = dot(u[...], mid[...].astype(BF16), ((0,), (0,))).astype(BF16)

        @pl.when(t == 0)
        def _():
            core_in[0] = jnp.zeros(core_out.shape, BF16)
            k_copy(core_out, 0).start()

        @pl.when(t == T - 1)
        def _():
            core_in[1] = jnp.zeros(core_out.shape, BF16)
            k_copy(core_out, 1).start()

    def make_left():
        core = core_in[0].astype(F32) + core_in[1].astype(F32) + core_out[...].astype(F32)
        core = (core * jnp.transpose(cb[me])[:, 2:3]).astype(BF16)
        mixed = row_base * mid[...] + dot(u[...], core)
        lall[me] = (mixed * dc).astype(BF16)
        loop(1, L, lambda d: l_copy(me, lax.rem(me + d, L)).start())

    sign = jnp.where(inner, -1.0, 1.0).astype(F32)

    def pushed(d):
        total = pin[d].astype(F32) + qin[d].astype(F32) + sign * own[d].astype(F32)
        return (total * jnp.transpose(cb[layer_of(d)])[:, 0:1]).astype(BF16)

    def update(l, block, basis, scaled, left):
        x = cb[l, 1:2, 0:1] * block.astype(F32)
        x = x + dot(basis, scaled)
        return x + dot(left, vall[l], ((1,), (1,)))

    def emit(d):
        l = layer_of(d)
        pl.when(d > 0)(lambda: l_copy(l, l).wait_recv())
        pl.when(t == T - 1)(lambda: p_copy(own.at[d], d).wait_recv())
        pl.when(t == 0)(lambda: q_copy(own.at[d], d).wait_recv())
        x = update(l, g[l], uall[l], pushed(d), lall[l])
        raw[l] = x.astype(BF16)
        nsend[1, pl.ds(l, 1), :] = lanes(x)

    final = L - 1
    lf = layer_of(final)

    def h_copies(side):
        to = lax.rem(t + (1 if side == 0 else T - 1), T)
        return [
            remote(src, dst, hs.at[k], hr.at[k], "tensor", to)
            for k, (src, dst) in enumerate(((g.at[lf], guest_g), (uall.at[lf], guest_u), (lall.at[lf], guest_l)))]

    def guest_emit():
        for copy in h_copies(0):
            copy.wait_recv()
        x = update(lf, guest_g[...], guest_u[...], pushed(final), guest_l[...])
        guest_x[...] = x.astype(BF16)
        guest_n[...] = lanes(x)
        pl.when(t == T - 2)(lambda: p_copy(guest_x, final).start())
        pl.when(t == 1)(lambda: q_copy(guest_x, final).start())

    blk = lax.rem(me, NP)
    home = lax.div(me, NP)
    dist = jnp.abs(t - home)
    third = -(-L // 3)
    first = jnp.where(dist == 0, 2 * blk + 4, blk * jnp.where(home < t, n_left, n_right) + dist + 2)
    at_core = NP * far + 2
    at_core_end = NP * (T - 1) + 2
    last = max(NP * (T - 2) + L, at_core_end + T - 2, NP * (T - 1) + 2, 2 * NP + 2)

    def step(s):
        relay(s, n_left, -1, 0, has_right)
        relay(s, n_right, 1, 1, has_left)
        pl.when(s == 1)(lambda: loop(0, NP, lambda i: spread(t, i)))
        pl.when(s < L)(lambda: end_send(s - 1))
        loop(jnp.clip(third * (s - 1) + 1, 1, L), jnp.clip(third * s + 1, 1, L), project)
        forward(s, t, p_copy, pin, 0)
        forward(s, T - 1 - t, q_copy, qin, 1)
        loop(jnp.where(s == first, 0, L), L, middle)

        @pl.when(s == at_core)
        def _():
            gather_middle()
            end_send(L - 1)

        pl.when(inner & (s == at_core_end + T - 2))(make_left)

    guest_n[...] = jnp.zeros_like(guest_n)
    nsend[1, pl.ds(lf, 1), :] = jnp.zeros((1, 128), F32)
    loop(1, last + 1, step)

    def end_left(side):
        copies = h_copies(side)
        copies[0].start()
        copies[1].start()
        core_pass(1 - side, False)
        make_left()
        l_copy(lf, lf).wait_recv()
        copies[2].start()

    pl.when(t == 0)(lambda: end_left(0))
    pl.when(t == T - 1)(lambda: end_left(1))
    pl.when((t == 1) | (t == T - 2))(guest_emit)
    loop(0, jnp.where(inner, L, L - 1), emit)

    nsend[1, pl.ds(lf, 1), :] = nsend[1, pl.ds(lf, 1), :] + guest_n[...]
    sums = jnp.sum(nsend[...], axis=2)
    tile[0:1, 0:L] = sums[0:1]
    tile[0:1, L:2 * L] = sums[1:2]

    def n_copy(slot, dst):
        return pltpu.make_async_remote_copy(
            src_ref=tile, dst_ref=nin.at[slot], send_sem=ns, recv_sem=nr,
            device_id={"layer": lax.div(dst, T), "tensor": lax.rem(dst, T)}, device_id_type=MESH)

    loop(1, N, lambda d: n_copy(here, lax.rem(here + d, N)).start())
    nin[here] = tile[...]

    def sent(ref, sem, axis):
        remote(ref, ref, sem, sem, axis, 0).wait_send()

    most = pl.ds(0, L - 1)
    for ref, sem in ((uall, us), (cb, bs), (vall, xs), (mout, ms), (lall, ls)):
        sent(ref.at[most], sem, "layer")
    pl.when(has_right)(lambda: k_copy(core_out, 0).wait_send())
    pl.when(has_left)(lambda: k_copy(core_out, 1).wait_send())

    pl.when(has_right)(lambda: sent(own, ps, "tensor"))
    pl.when(has_left)(lambda: sent(own, qs, "tensor"))

    def drain_v(c):
        pl.when((c <= t) & has_right)(lambda: sent(vline.at[c], vs.at[0, c], "tensor"))
        pl.when((c >= t) & has_left)(lambda: sent(vline.at[c], vs.at[1, c], "tensor"))

    loop(0, T, drain_v)

    for side, end in ((0, 0), (1, T - 1)):
        @pl.when(t == end)
        def _(side=side):
            for copy in h_copies(side):
                copy.wait_send()

    arrived = remote(nin.at[pl.ds(0, N - 1)], nin.at[pl.ds(0, N - 1)], ns, nr, "layer", 0)
    arrived.wait_recv()
    tot = jnp.sum(nin[...], axis=0)
    fac = jnp.sqrt((tot[:, 0:L] + 1.0) / (tot[:, L:2 * L] + 1.0))
    factor[...] = jnp.broadcast_to(jnp.transpose(jnp.broadcast_to(fac, (8, L)))[:, 0:1], factor.shape)

    arrived.wait_send()

    @pl.when(t == T - 1)
    def _():
        p_copy(own.at[final], final).wait_recv()
        raw[lf] = pin[final]

    @pl.when(t == 0)
    def _():
        q_copy(own.at[final], final).wait_recv()
        raw[lf] = qin[final]


def scale_kernel(raw, factor, out, buf, sem):
    def one(l):
        buf[l] = (raw[l].astype(F32) * factor[pl.ds(l, 1), 0:1]).astype(BF16)
        pltpu.make_async_copy(buf.at[l], out.at[l], sem.at[l]).start()

    L = raw.shape[0]
    loop(0, L, one)
    loop(0, L, lambda l: pltpu.make_async_copy(buf.at[l], out.at[l], sem.at[l]).wait())


def solution(mesh):
    L, T = mesh.shape["layer"], mesh.shape["tensor"]
    NP = L // T

    def body(gradient, row_basis, column_basis, row_eigen, column_eigen, row_escape, column_escape):
        _, r, W = gradient.shape
        _, Cr, K = column_basis.shape
        vmem = pl.BlockSpec(memory_space=pltpu.VMEM)
        hbm = pl.BlockSpec(memory_space=pl.ANY)
        chunk = pltpu.VMEM((L, K, W), BF16)
        small = pltpu.VMEM((L, r, K), BF16)
        sem = pltpu.SemaphoreType.DMA
        raw, factor = pl.pallas_call(
            functools.partial(kernel, L, T, NP),
            out_shape=(pltpu.VMEM((L, r, W), BF16), pltpu.VMEM((L, 128), F32)),
            in_specs=[hbm, vmem, hbm, vmem, vmem, vmem, vmem],
            out_specs=(vmem, vmem),
            scratch_shapes=[
                pltpu.VMEM((L, r, W), BF16),
                small,
                pltpu.VMEM((L, W, K), BF16),
                pltpu.VMEM((T, NP, Cr // NP, K), BF16),
                chunk, chunk, chunk,
                small, small,
                pltpu.VMEM((r, K), F32),
                small,
                pltpu.VMEM((K, K), BF16),
                pltpu.VMEM((2, K, K), BF16),
                pltpu.VMEM((2, K, K), BF16),
                pltpu.VMEM((L, 8, K), F32),
                pltpu.VMEM((r, W), BF16),
                pltpu.VMEM((r, K), BF16),
                pltpu.VMEM((r, K), BF16),
                pltpu.VMEM((r, W), BF16),
                pltpu.VMEM((1, 128), F32),
                pltpu.VMEM((2, L, 128), F32),
                pltpu.VMEM((1, 128), F32),
                pltpu.VMEM((L * T, 1, 128), F32),
                sem, sem((L,)),
                sem, sem((L,)),
                sem((2, T)), sem((T, NP)),
                sem, sem((L,)),
                sem, sem,
                sem((2,)), sem((2,)),
                sem, sem((L,)),
                sem, sem((L,)),
                sem, sem((L,)),
                sem, sem,
                sem((3,)), sem((3,)),
                sem, sem((NP,)),
            ],
            compiler_params=pltpu.CompilerParams(
                collective_id=0, has_side_effects=True, vmem_limit_bytes=67043328 - 2 * L * r * W - 256 * 1024),
        )(gradient, row_basis[0], column_basis[0], row_eigen, column_eigen,
          row_escape[:, None], column_escape[:, None])
        return pl.pallas_call(
            scale_kernel,
            out_shape=jax.ShapeDtypeStruct((L, r, W), BF16),
            in_specs=[vmem, vmem],
            out_specs=hbm,
            scratch_shapes=[pltpu.VMEM((L, r, W), BF16), sem((L,))],
            compiler_params=pltpu.CompilerParams(vmem_limit_bytes=32 * 1024 * 1024),
        )(raw, factor)

    in_specs = (
        P(None, "tensor", "layer"),
        P("layer", "tensor", None),
        P("layer", "tensor", None),
        P("layer", None),
        P("layer", None),
        P("layer"),
        P("layer"),
    )
    out_specs = P(None, "tensor", "layer")
    return jax.shard_map(body, mesh=mesh, in_specs=in_specs, out_specs=out_specs, check_vma=False)
```

```python
import functools

import jax
import jax.numpy as jnp
from jax import lax
from jax.experimental import pallas as pl
from jax.experimental.pallas import tpu as pltpu
from jax.sharding import PartitionSpec as P

MESH = pl.DeviceIdType.MESH
F32 = jnp.float32
BF16 = jnp.bfloat16


def remote(src, dst, send, recv, axis, index):
    return pltpu.make_async_remote_copy(
        src_ref=src,
        dst_ref=dst,
        send_sem=send,
        recv_sem=recv,
        device_id={axis: index},
        device_id_type=MESH,
    )


def loop(lo, hi, fn):
    def step(i, carry):
        fn(i)
        return carry

    lax.fori_loop(lo, hi, step, 0)


def dot(a, b, dims=((1,), (0,))):
    return lax.dot_general(a, b, (dims, ((), ())), preferred_element_type=F32)


def quarter(x):
    return lax.rsqrt(jnp.sqrt(x))


def lanes(x):
    s = jnp.sum(x * x, axis=0, keepdims=True)
    out = s[:, 0:128]
    for k in range(1, x.shape[1] // 128):
        out = out + s[:, k * 128:(k + 1) * 128]
    return out


def kernel(
    L, T, NP,
    g_hbm, u_hbm, cols_hbm, reig_hbm, ceig_hbm, resc_hbm, cesc_hbm,
    raw,
    g, u, reig, ceig, resc, cesc, uall, vall, vline, own, pin, qin, mout, mi, mid, lall, core_out, core_in, core_sum, cb,
    guest_g, guest_u, guest_l, guest_x, guest_n, nsend, tile, nin, factor,
    us, ur, bs, br, vs, vr, xs, xr, ms, mr, ks, kr, ls, lr, ps, pr, qs, qr, ns, nr, hs, hr, gs, cs, es,
):
    me = lax.axis_index("layer")
    t = lax.axis_index("tensor")
    W = g.shape[2]
    K = u.shape[1]
    right, lft = t + 1, t - 1
    has_right, has_left = t < T - 1, t > 0
    inner = has_right & has_left
    far = jnp.maximum(t, T - 1 - t)
    n_left, n_right = t, T - 1 - t

    here = me * T + t
    N = L * T

    g_in = pltpu.make_async_copy(g_hbm, g, gs)
    small_in = [pltpu.make_async_copy(src, dst, es.at[k]) for k, (src, dst) in enumerate((
        (u_hbm, u), (reig_hbm, reig), (ceig_hbm, ceig), (resc_hbm, resc), (cesc_hbm, cesc)))]

    def cols_in(i):
        return pltpu.make_async_copy(cols_hbm.at[pl.ds(i * W, W)], vline.at[t, i], cs.at[i])

    for i in range(NP):
        cols_in(i).start()

    def greet(axis, index):
        pl.semaphore_signal(barrier, inc=1, device_id={axis: index}, device_id_type=MESH)

    barrier = pltpu.get_barrier_semaphore()
    pl.when(has_right)(lambda: greet("tensor", right))
    pl.when(has_left)(lambda: greet("tensor", lft))
    loop(1, L, lambda d: greet("layer", lax.rem(me + d, L)))
    for copy in small_in:
        copy.start()
    g_in.start()
    for i in range(NP):
        cols_in(i).wait()
    pl.semaphore_wait(barrier, L - 1 + jnp.where(inner, 2, 1))

    def layer_of(d):
        return lax.rem(me + d, L)

    def v_copy(src, c, i, side):
        return remote(src, vline.at[c, i], vs.at[side, c], vr.at[c, i], "tensor",
                      right if side == 0 else lft)

    def x_copy(src, slot, dst):
        return remote(src, vall.at[slot], xs, xr.at[slot], "layer", dst)

    def u_copy(slot, dst):
        return remote(u, uall.at[slot], us, ur.at[slot], "layer", dst)

    def b_copy(slot, dst):
        return remote(cb.at[me], cb.at[slot], bs, br.at[slot], "layer", dst)

    def m_copy(slot, dst):
        return remote(mout.at[dst], mi.at[slot], ms, mr, "layer", dst)

    def l_copy(slot, dst):
        return remote(lall.at[me], lall.at[slot], ls, lr.at[slot], "layer", dst)

    def k_copy(src, side):
        return remote(src, core_in.at[side], ks.at[side], kr.at[side], "tensor", right if side == 0 else lft)

    def p_copy(src, d):
        return remote(src, pin.at[d], ps, pr.at[d], "tensor", right)

    def q_copy(src, d):
        return remote(src, qin.at[d], qs, qr.at[d], "tensor", lft)

    def send_own(i, side):
        v_copy(vline.at[t, i], t, i, side).start()

    def send_half(i, half, side):
        rows = vline.at[t, i, pl.ds(half * (W // 2), W // 2)]
        remote(rows, rows, vs.at[side, t], vr.at[t, i], "tensor", right if side == 0 else lft).start()

    def send_first(side, onward, n):
        @pl.when(onward)
        def _():
            loop(0, jnp.where(n > 0, 1, NP), lambda i: send_own(i, side))
            pl.when((n > 0) & (NP > 1))(lambda: send_half(1, 0, side))

    send_first(0, has_right, n_left)
    send_first(1, has_left, n_right)
    for copy in small_in:
        copy.wait()
    tile[...] = jnp.zeros_like(tile)
    row_base = quarter(resc[...])
    column_base = quarter(cesc[...])
    row_coef = quarter(reig[...] + resc[...]) - row_base
    dc = quarter(ceig[...] + cesc[...]) - column_base
    cb[me, 0:1, :] = row_coef * column_base
    cb[me, 1:2, :] = jnp.broadcast_to(row_base * column_base, (1, K))
    cb[me, 2:8, :] = jnp.broadcast_to(row_coef, (6, K))
    uall[me] = u[...]

    def send_basis(d):
        dst = lax.rem(me - d + L, L)
        u_copy(me, dst).start()
        b_copy(me, dst).start()

    loop(1, L, send_basis)

    def spread(c, i):
        dst = c * NP + i
        pl.when(dst != me)(lambda: x_copy(vline.at[c, i], me, dst).start())

        @pl.when(dst == me)
        def _():
            vall[me] = vline[c, i]

    @pl.when(t == 0)
    def _():
        loop(0, L, lambda d: pin.__setitem__(d, jnp.zeros(pin.shape[1:], BF16)))

    @pl.when(t == T - 1)
    def _():
        loop(0, L, lambda d: qin.__setitem__(d, jnp.zeros(qin.shape[1:], BF16)))

    def project(d):
        l = layer_of(d)

        @pl.when(d > 0)
        def _():
            u_copy(l, l).wait_recv()
            b_copy(l, l).wait_recv()

        block = g[l]
        own[d] = dot(uall[l], block, ((0,), (0,))).astype(BF16)
        nsend[0, pl.ds(l, 1), :] = lanes(block.astype(F32))

    g_in.wait()
    project(0)

    def end_send(d):
        @pl.when((d >= 0) & (d < L))
        def _():
            pl.when(t == 0)(lambda: p_copy(own.at[d], d).start())
            pl.when(t == T - 1)(lambda: q_copy(own.at[d], d).start())

    def core_pass(side, onward):
        k_copy(core_out, side).wait_recv()

        @pl.when(onward)
        def _():
            core_sum[side] = (core_in[side].astype(F32) + core_out[...].astype(F32)).astype(BF16)
            k_copy(core_sum.at[side], side).start()

    def forward(s, tau, copy, buf, side):
        d = s - NP * tau - 1
        ok = (d >= 0) & (d < L) & inner
        pl.when(ok)(lambda: copy(own.at[0], d).wait_recv())
        pl.when(inner & (s == at_core_end + tau))(lambda: core_pass(side, True))

        @pl.when(ok)
        def _():
            buf[d] = (buf[d].astype(F32) + own[d].astype(F32)).astype(BF16)
            pl.when((d < L - 1) | (tau < T - 2))(lambda: copy(buf.at[d], d).start())

    def relay(s, n, way, side, onward):
        near = jnp.maximum(n, 1)
        i, h = lax.div(s - 1, near), lax.rem(s - 1, near) + 1
        c = t + way * h

        @pl.when(s <= NP * n)
        def _():
            v_copy(vline.at[c, i], c, i, side).wait_recv()
            pl.when(onward)(lambda: v_copy(vline.at[c, i], c, i, side).start())
            pl.when(onward & (h == 1) & (i + 1 < NP))(lambda: send_half(i + 1, 1, side))
            pl.when(onward & (h == n) & (i + 2 < NP))(lambda: send_half(i + 2, 0, side))
            spread(c, i)

    def middle(d):
        l = layer_of(d)
        pl.when(d > 0)(lambda: x_copy(vall.at[l], l, l).wait_recv())
        m = dot(g[l], vall[l]).astype(BF16)

        @pl.when(d == 0)
        def _():
            mi[me] = m

        @pl.when(d > 0)
        def _():
            mout[l] = m
            m_copy(me, l).start()

    def gather_middle():
        total = mi[me].astype(F32)
        mid[...] = total

        remote(mout.at[pl.ds(0, L - 1)], mi.at[pl.ds(0, L - 1)], ms, mr, "layer", me).wait_recv()

        def add(d):
            mid[...] += mi[layer_of(d)].astype(F32)

        loop(1, L, add)
        core_out[...] = dot(u[...], mid[...].astype(BF16), ((0,), (0,))).astype(BF16)

        @pl.when(t == 0)
        def _():
            core_in[0] = jnp.zeros(core_out.shape, BF16)
            k_copy(core_out, 0).start()

        @pl.when(t == T - 1)
        def _():
            core_in[1] = jnp.zeros(core_out.shape, BF16)
            k_copy(core_out, 1).start()

    def make_left():
        core = core_in[0].astype(F32) + core_in[1].astype(F32) + core_out[...].astype(F32)
        core = (core * jnp.transpose(cb[me])[:, 2:3]).astype(BF16)
        mixed = row_base * mid[...] + dot(u[...], core)
        lall[me] = (mixed * dc).astype(BF16)
        loop(1, L, lambda d: l_copy(me, lax.rem(me + d, L)).start())

    sign = jnp.where(inner, -1.0, 1.0).astype(F32)

    def pushed(d):
        total = pin[d].astype(F32) + qin[d].astype(F32) + sign * own[d].astype(F32)
        return (total * jnp.transpose(cb[layer_of(d)])[:, 0:1]).astype(BF16)

    def update(l, block, basis, scaled, left):
        x = cb[l, 1:2, 0:1] * block.astype(F32)
        x = x + dot(basis, scaled)
        return x + dot(left, vall[l], ((1,), (1,)))

    def emit(d):
        l = layer_of(d)
        pl.when(d > 0)(lambda: l_copy(l, l).wait_recv())
        pl.when(t == T - 1)(lambda: p_copy(own.at[d], d).wait_recv())
        pl.when(t == 0)(lambda: q_copy(own.at[d], d).wait_recv())
        x = update(l, g[l], uall[l], pushed(d), lall[l])
        raw[l] = x.astype(BF16)
        nsend[1, pl.ds(l, 1), :] = lanes(x)

    final = L - 1
    lf = layer_of(final)

    def h_copies(side):
        to = lax.rem(t + (1 if side == 0 else T - 1), T)
        return [
            remote(src, dst, hs.at[k], hr.at[k], "tensor", to)
            for k, (src, dst) in enumerate(((g.at[lf], guest_g), (uall.at[lf], guest_u), (lall.at[lf], guest_l)))]

    def guest_emit():
        for copy in h_copies(0):
            copy.wait_recv()
        x = update(lf, guest_g[...], guest_u[...], pushed(final), guest_l[...])
        guest_x[...] = x.astype(BF16)
        guest_n[...] = lanes(x)

    blk = lax.rem(me, NP)
    home = lax.div(me, NP)
    dist = jnp.abs(t - home)
    third = -(-L // 3)
    first = jnp.where(dist == 0, 2 * blk + 4, blk * jnp.where(home < t, n_left, n_right) + dist + 2)
    at_core = NP * far + 2
    at_core_end = NP * (T - 1) + 2
    last = max(NP * (T - 2) + L, at_core_end + T - 2, NP * (T - 1) + 2, 2 * NP + 2)

    def step(s):
        relay(s, n_left, -1, 0, has_right)
        relay(s, n_right, 1, 1, has_left)
        pl.when(s == 1)(lambda: loop(0, NP, lambda i: spread(t, i)))
        pl.when(s < L)(lambda: end_send(s - 1))
        loop(jnp.clip(third * (s - 1) + 1, 1, L), jnp.clip(third * s + 1, 1, L), project)
        forward(s, t, p_copy, pin, 0)
        forward(s, T - 1 - t, q_copy, qin, 1)
        loop(jnp.where(s == first, 0, L), L, middle)

        @pl.when(s == at_core)
        def _():
            gather_middle()
            end_send(L - 1)

        pl.when(inner & (s == at_core_end + T - 2))(make_left)

    guest_n[...] = jnp.zeros_like(guest_n)
    nsend[1, pl.ds(lf, 1), :] = jnp.zeros((1, 128), F32)
    loop(1, last + 1, step)

    def end_left(side):
        copies = h_copies(side)
        copies[0].start()
        copies[1].start()
        core_pass(1 - side, False)
        make_left()
        l_copy(lf, lf).wait_recv()
        copies[2].start()

    pl.when(t == 0)(lambda: end_left(0))
    pl.when(t == T - 1)(lambda: end_left(1))
    pl.when((t == 1) | (t == T - 2))(guest_emit)
    loop(0, jnp.where(inner, L, L - 1), emit)

    nsend[1, pl.ds(lf, 1), :] = nsend[1, pl.ds(lf, 1), :] + guest_n[...]
    sums = jnp.sum(nsend[...], axis=2)
    tile[0:1, 0:L] = sums[0:1]
    tile[0:1, L:2 * L] = sums[1:2]

    def n_copy(slot, dst):
        return pltpu.make_async_remote_copy(
            src_ref=tile, dst_ref=nin.at[slot], send_sem=ns, recv_sem=nr,
            device_id={"layer": lax.div(dst, T), "tensor": lax.rem(dst, T)}, device_id_type=MESH)

    loop(1, N, lambda d: n_copy(here, lax.rem(here + d, N)).start())
    pl.when(t == T - 2)(lambda: p_copy(guest_x, final).start())
    pl.when(t == 1)(lambda: q_copy(guest_x, final).start())
    nin[here] = tile[...]

    def sent(ref, sem, axis):
        remote(ref, ref, sem, sem, axis, 0).wait_send()

    most = pl.ds(0, L - 1)
    for ref, sem in ((uall, us), (cb, bs), (vall, xs), (mout, ms), (lall, ls)):
        sent(ref.at[most], sem, "layer")
    pl.when(has_right)(lambda: k_copy(core_out, 0).wait_send())
    pl.when(has_left)(lambda: k_copy(core_out, 1).wait_send())

    pl.when(has_right)(lambda: sent(own, ps, "tensor"))
    pl.when(has_left)(lambda: sent(own, qs, "tensor"))

    def drain_v(c):
        pl.when((c <= t) & has_right)(lambda: sent(vline.at[c], vs.at[0, c], "tensor"))
        pl.when((c >= t) & has_left)(lambda: sent(vline.at[c], vs.at[1, c], "tensor"))

    loop(0, T, drain_v)

    for side, end in ((0, 0), (1, T - 1)):
        @pl.when(t == end)
        def _(side=side):
            for copy in h_copies(side):
                copy.wait_send()

    arrived = remote(nin.at[pl.ds(0, N - 1)], nin.at[pl.ds(0, N - 1)], ns, nr, "layer", 0)
    arrived.wait_recv()
    tot = jnp.sum(nin[...], axis=0)
    fac = jnp.sqrt((tot[:, 0:L] + 1.0) / (tot[:, L:2 * L] + 1.0))
    factor[...] = jnp.broadcast_to(jnp.transpose(jnp.broadcast_to(fac, (8, L)))[:, 0:1], factor.shape)
    arrived.wait_send()

    def scale(l, rows):
        raw[l] = (rows.astype(F32) * factor[pl.ds(l, 1), 0:1]).astype(BF16)

    def rescale(d):
        l = layer_of(d)
        scale(l, raw[l])

    loop(0, jnp.where(inner, L, L - 1), rescale)

    @pl.when(t == T - 1)
    def _():
        p_copy(own.at[final], final).wait_recv()
        scale(lf, pin[final])

    @pl.when(t == 0)
    def _():
        q_copy(own.at[final], final).wait_recv()
        scale(lf, qin[final])


def solution(mesh):
    L, T = mesh.shape["layer"], mesh.shape["tensor"]
    NP = L // T

    def body(gradient, row_basis, column_basis, row_eigen, column_eigen, row_escape, column_escape):
        _, r, W = gradient.shape
        _, Cr, K = column_basis.shape
        vmem = pl.BlockSpec(memory_space=pltpu.VMEM)
        hbm = pl.BlockSpec(memory_space=pl.ANY)
        chunk = pltpu.VMEM((L, K, W), BF16)
        small = pltpu.VMEM((L, r, K), BF16)
        sem = pltpu.SemaphoreType.DMA
        rows = pl.pallas_call(
            functools.partial(kernel, L, T, NP),
            out_shape=pltpu.VMEM((L, r, W), BF16),
            in_specs=[hbm] * 7,
            out_specs=vmem,
            scratch_shapes=[
                pltpu.VMEM((L, r, W), BF16),
                pltpu.VMEM((r, K), BF16),
                pltpu.VMEM((1, K), F32), pltpu.VMEM((1, K), F32),
                pltpu.VMEM((1, 1), F32), pltpu.VMEM((1, 1), F32),
                small,
                pltpu.VMEM((L, W, K), BF16),
                pltpu.VMEM((T, NP, Cr // NP, K), BF16),
                chunk, chunk, chunk,
                small, small,
                pltpu.VMEM((r, K), F32),
                small,
                pltpu.VMEM((K, K), BF16),
                pltpu.VMEM((2, K, K), BF16),
                pltpu.VMEM((2, K, K), BF16),
                pltpu.VMEM((L, 8, K), F32),
                pltpu.VMEM((r, W), BF16),
                pltpu.VMEM((r, K), BF16),
                pltpu.VMEM((r, K), BF16),
                pltpu.VMEM((r, W), BF16),
                pltpu.VMEM((1, 128), F32),
                pltpu.VMEM((2, L, 128), F32),
                pltpu.VMEM((1, 128), F32),
                pltpu.VMEM((L * T, 1, 128), F32),
                pltpu.VMEM((L, 128), F32),
                sem, sem((L,)),
                sem, sem((L,)),
                sem((2, T)), sem((T, NP)),
                sem, sem((L,)),
                sem, sem,
                sem((2,)), sem((2,)),
                sem, sem((L,)),
                sem, sem((L,)),
                sem, sem((L,)),
                sem, sem,
                sem((3,)), sem((3,)),
                sem, sem((NP,)), sem((5,)),
            ],
            compiler_params=pltpu.CompilerParams(
                collective_id=0, has_side_effects=True, vmem_limit_bytes=67043328 - 2 * L * r * W - 256 * 1024),
        )(gradient, row_basis[0], column_basis[0], row_eigen, column_eigen,
          row_escape[:, None], column_escape[:, None])
        return rows

    in_specs = (
        P(None, "tensor", "layer"),
        P("layer", "tensor", None),
        P("layer", "tensor", None),
        P("layer", None),
        P("layer", None),
        P("layer"),
        P("layer"),
    )
    out_specs = P(None, "tensor", "layer")
    return jax.shard_map(body, mesh=mesh, in_specs=in_specs, out_specs=out_specs, check_vma=False)
```

```python
import functools

import jax
import jax.numpy as jnp
from jax import lax
from jax.experimental import pallas as pl
from jax.experimental.pallas import tpu as pltpu
from jax.sharding import PartitionSpec as P

MESH = pl.DeviceIdType.MESH
F32 = jnp.float32
BF16 = jnp.bfloat16


def remote(src, dst, send, recv, axis, index):
    return pltpu.make_async_remote_copy(
        src_ref=src,
        dst_ref=dst,
        send_sem=send,
        recv_sem=recv,
        device_id={axis: index},
        device_id_type=MESH,
    )


def loop(lo, hi, fn):
    def step(i, carry):
        fn(i)
        return carry

    lax.fori_loop(lo, hi, step, 0)


def dot(a, b, dims=((1,), (0,))):
    return lax.dot_general(a, b, (dims, ((), ())), preferred_element_type=F32)


def quarter(x):
    return lax.rsqrt(jnp.sqrt(x))


def lanes(x):
    s = jnp.sum(x * x, axis=0, keepdims=True)
    out = s[:, 0:128]
    for k in range(1, x.shape[1] // 128):
        out = out + s[:, k * 128:(k + 1) * 128]
    return out


def kernel(
    L, T, NP,
    g_hbm, u_hbm, cols_hbm, reig_hbm, ceig_hbm, resc_hbm, cesc_hbm,
    raw,
    g, u, reig, ceig, resc, cesc, uall, vall, vline, own, pin, qin, mout, mi, mid, lall, core_out, core_in, core_sum, cb,
    guest_g, guest_u, guest_l, guest_x, guest_n, nsend, tile, nin, factor,
    us, ur, bs, br, vs, vr, xs, xr, ms, mr, ks, kr, ls, lr, ps, pr, qs, qr, ns, nr, hs, hr, gs, cs, es,
):
    me = lax.axis_index("layer")
    t = lax.axis_index("tensor")
    W = g.shape[2]
    K = u.shape[1]
    right, lft = t + 1, t - 1
    has_right, has_left = t < T - 1, t > 0
    inner = has_right & has_left
    far = jnp.maximum(t, T - 1 - t)
    n_left, n_right = t, T - 1 - t

    here = me * T + t
    N = L * T

    g_in = pltpu.make_async_copy(g_hbm, g, gs)
    small_in = [pltpu.make_async_copy(src, dst, es.at[k]) for k, (src, dst) in enumerate((
        (u_hbm, u), (reig_hbm, reig), (ceig_hbm, ceig), (resc_hbm, resc), (cesc_hbm, cesc)))]

    def cols_in(i):
        return pltpu.make_async_copy(cols_hbm.at[pl.ds(i * W, W)], vline.at[t, i], cs.at[i])

    for i in range(NP):
        cols_in(i).start()

    bits = [1 << b for b in range(L.bit_length() - 1)]

    def masks(k):
        return [mask for mask in range(1, L) if bin(mask).count("1") == k]

    def partner(mask):
        index = me
        for b in bits:
            if mask & b:
                index = index + b - 2 * b * lax.rem(lax.div(me, b), 2)
        return index

    def greet(axis, index):
        pl.semaphore_signal(barrier, inc=1, device_id={axis: index}, device_id_type=MESH)

    barrier = pltpu.get_barrier_semaphore()
    pl.when(has_right)(lambda: greet("tensor", right))
    pl.when(has_left)(lambda: greet("tensor", lft))
    for mask in masks(1):
        greet("layer", partner(mask))
    for copy in small_in:
        copy.start()
    g_in.start()
    for i in range(NP):
        cols_in(i).wait()
    pl.semaphore_wait(barrier, len(bits) + jnp.where(inner, 2, 1))

    def layer_of(d):
        return lax.rem(me + d, L)

    def v_copy(src, c, i, side):
        return remote(src, vline.at[c, i], vs.at[side, c], vr.at[c, i], "tensor",
                      right if side == 0 else lft)

    def x_copy(src, slot, dst):
        return remote(src, vall.at[slot], xs, xr.at[slot], "layer", dst)

    def u_copy(slot, dst):
        return remote(u, uall.at[slot], us, ur.at[slot], "layer", dst)

    def b_copy(slot, dst):
        return remote(cb.at[me], cb.at[slot], bs, br.at[slot], "layer", dst)

    def m_copy(slot, dst):
        return remote(mout.at[dst], mi.at[slot], ms, mr, "layer", dst)

    def l_copy(slot, dst):
        return remote(lall.at[me], lall.at[slot], ls, lr.at[slot], "layer", dst)

    def k_copy(src, side):
        return remote(src, core_in.at[side], ks.at[side], kr.at[side], "tensor", right if side == 0 else lft)

    def p_copy(src, d):
        return remote(src, pin.at[d], ps, pr.at[d], "tensor", right)

    def q_copy(src, d):
        return remote(src, qin.at[d], qs, qr.at[d], "tensor", lft)

    def send_own(i, side):
        v_copy(vline.at[t, i], t, i, side).start()

    def send_half(i, half, side):
        rows = vline.at[t, i, pl.ds(half * (W // 2), W // 2)]
        remote(rows, rows, vs.at[side, t], vr.at[t, i], "tensor", right if side == 0 else lft).start()

    def send_first(side, onward, n):
        @pl.when(onward)
        def _():
            loop(0, jnp.where(n > 0, 1, NP), lambda i: send_own(i, side))
            pl.when((n > 0) & (NP > 1))(lambda: send_half(1, 0, side))

    send_first(0, has_right, n_left)
    send_first(1, has_left, n_right)
    for copy in small_in:
        copy.wait()
    tile[...] = jnp.zeros_like(tile)
    row_base = quarter(resc[...])
    column_base = quarter(cesc[...])
    row_coef = quarter(reig[...] + resc[...]) - row_base
    dc = quarter(ceig[...] + cesc[...]) - column_base
    cb[me, 0:1, :] = row_coef * column_base
    cb[me, 1:2, :] = jnp.broadcast_to(row_base * column_base, (1, K))
    cb[me, 2:8, :] = jnp.broadcast_to(row_coef, (6, K))
    uall[me] = u[...]

    def send_basis(mask):
        dst = partner(mask)
        u_copy(me, dst).start()
        b_copy(me, dst).start()

    def take_basis(mask):
        src = partner(mask)
        u_copy(src, src).wait_recv()

    for mask in masks(1):
        send_basis(mask)

    def spread(c, i):
        dst = c * NP + i
        pl.when(dst != me)(lambda: x_copy(vline.at[c, i], me, dst).start())

        @pl.when(dst == me)
        def _():
            vall[me] = vline[c, i]

    @pl.when(t == 0)
    def _():
        loop(0, L, lambda d: pin.__setitem__(d, jnp.zeros(pin.shape[1:], BF16)))

    @pl.when(t == T - 1)
    def _():
        loop(0, L, lambda d: qin.__setitem__(d, jnp.zeros(qin.shape[1:], BF16)))

    def project(d):
        l = layer_of(d)

        @pl.when(d > 0)
        def _():
            b_copy(l, l).wait_recv()

        block = g[l]
        own[d] = dot(uall[l], block, ((0,), (0,))).astype(BF16)
        nsend[0, pl.ds(l, 1), :] = lanes(block.astype(F32))

    g_in.wait()
    project(0)
    for k in range(1, len(bits)):
        for mask in masks(k):
            take_basis(mask)
        for mask in masks(k + 1):
            send_basis(mask)

    def end_send(d):
        @pl.when((d >= 0) & (d < L))
        def _():
            pl.when(t == 0)(lambda: p_copy(own.at[d], d).start())
            pl.when(t == T - 1)(lambda: q_copy(own.at[d], d).start())

    def core_pass(side, onward):
        k_copy(core_out, side).wait_recv()

        @pl.when(onward)
        def _():
            core_sum[side] = (core_in[side].astype(F32) + core_out[...].astype(F32)).astype(BF16)
            k_copy(core_sum.at[side], side).start()

    def forward(s, tau, copy, buf, side):
        d = s - NP * tau - 1
        ok = (d >= 0) & (d < L) & inner
        pl.when(ok)(lambda: copy(own.at[0], d).wait_recv())
        pl.when(inner & (s == at_core_end + tau))(lambda: core_pass(side, True))

        @pl.when(ok)
        def _():
            buf[d] = (buf[d].astype(F32) + own[d].astype(F32)).astype(BF16)
            pl.when((d < L - 1) | (tau < T - 2))(lambda: copy(buf.at[d], d).start())

    def relay(s, n, way, side, onward):
        near = jnp.maximum(n, 1)
        i, h = lax.div(s - 1, near), lax.rem(s - 1, near) + 1
        c = t + way * h

        @pl.when(s <= NP * n)
        def _():
            v_copy(vline.at[c, i], c, i, side).wait_recv()
            pl.when(onward)(lambda: v_copy(vline.at[c, i], c, i, side).start())
            pl.when(onward & (h == 1) & (i + 1 < NP))(lambda: send_half(i + 1, 1, side))
            pl.when(onward & (h == n) & (i + 2 < NP))(lambda: send_half(i + 2, 0, side))
            spread(c, i)

    def middle(d):
        l = layer_of(d)
        pl.when(d > 0)(lambda: x_copy(vall.at[l], l, l).wait_recv())
        m = dot(g[l], vall[l]).astype(BF16)

        @pl.when(d == 0)
        def _():
            mi[me] = m

        @pl.when(d > 0)
        def _():
            mout[l] = m
            m_copy(me, l).start()

    def gather_middle():
        total = mi[me].astype(F32)
        mid[...] = total

        remote(mout.at[pl.ds(0, L - 1)], mi.at[pl.ds(0, L - 1)], ms, mr, "layer", me).wait_recv()

        def add(d):
            mid[...] += mi[layer_of(d)].astype(F32)

        loop(1, L, add)
        core_out[...] = dot(u[...], mid[...].astype(BF16), ((0,), (0,))).astype(BF16)

        @pl.when(t == 0)
        def _():
            core_in[0] = jnp.zeros(core_out.shape, BF16)
            k_copy(core_out, 0).start()

        @pl.when(t == T - 1)
        def _():
            core_in[1] = jnp.zeros(core_out.shape, BF16)
            k_copy(core_out, 1).start()

    def make_left():
        core = core_in[0].astype(F32) + core_in[1].astype(F32) + core_out[...].astype(F32)
        core = (core * jnp.transpose(cb[me])[:, 2:3]).astype(BF16)
        mixed = row_base * mid[...] + dot(u[...], core)
        lall[me] = (mixed * dc).astype(BF16)
        loop(1, L, lambda d: l_copy(me, lax.rem(me + d, L)).start())

    sign = jnp.where(inner, -1.0, 1.0).astype(F32)

    def pushed(d):
        total = pin[d].astype(F32) + qin[d].astype(F32) + sign * own[d].astype(F32)
        return (total * jnp.transpose(cb[layer_of(d)])[:, 0:1]).astype(BF16)

    def update(l, block, basis, scaled, left):
        x = cb[l, 1:2, 0:1] * block.astype(F32)
        x = x + dot(basis, scaled)
        return x + dot(left, vall[l], ((1,), (1,)))

    def emit(d):
        l = layer_of(d)
        pl.when(d > 0)(lambda: l_copy(l, l).wait_recv())
        pl.when(t == T - 1)(lambda: p_copy(own.at[d], d).wait_recv())
        pl.when(t == 0)(lambda: q_copy(own.at[d], d).wait_recv())
        x = update(l, g[l], uall[l], pushed(d), lall[l])
        raw[l] = x.astype(BF16)
        nsend[1, pl.ds(l, 1), :] = lanes(x)

    final = L - 1
    lf = layer_of(final)

    def h_copies(side):
        to = lax.rem(t + (1 if side == 0 else T - 1), T)
        return [
            remote(src, dst, hs.at[k], hr.at[k], "tensor", to)
            for k, (src, dst) in enumerate(((g.at[lf], guest_g), (uall.at[lf], guest_u), (lall.at[lf], guest_l)))]

    def guest_emit():
        for copy in h_copies(0):
            copy.wait_recv()
        x = update(lf, guest_g[...], guest_u[...], pushed(final), guest_l[...])
        guest_x[...] = x.astype(BF16)
        guest_n[...] = lanes(x)

    blk = lax.rem(me, NP)
    home = lax.div(me, NP)
    dist = jnp.abs(t - home)
    third = -(-L // 3)
    first = jnp.where(dist == 0, 2 * blk + 4, blk * jnp.where(home < t, n_left, n_right) + dist + 2)
    at_core = NP * far + 2
    at_core_end = NP * (T - 1) + 2
    last = max(NP * (T - 2) + L, at_core_end + T - 2, NP * (T - 1) + 2, 2 * NP + 2)

    def step(s):
        relay(s, n_left, -1, 0, has_right)
        relay(s, n_right, 1, 1, has_left)
        pl.when(s == 1)(lambda: loop(0, NP, lambda i: spread(t, i)))
        pl.when(s < L)(lambda: end_send(s - 1))
        pl.when(s == 1)(lambda: take_basis(L - 1))
        loop(jnp.clip(third * (s - 1) + 1, 1, L), jnp.clip(third * s + 1, 1, L), project)
        forward(s, t, p_copy, pin, 0)
        forward(s, T - 1 - t, q_copy, qin, 1)
        loop(jnp.where(s == first, 0, L), L, middle)

        @pl.when(s == at_core)
        def _():
            gather_middle()
            end_send(L - 1)

        pl.when(inner & (s == at_core_end + T - 2))(make_left)

    guest_n[...] = jnp.zeros_like(guest_n)
    nsend[1, pl.ds(lf, 1), :] = jnp.zeros((1, 128), F32)
    loop(1, last + 1, step)

    def end_left(side):
        copies = h_copies(side)
        copies[0].start()
        copies[1].start()
        core_pass(1 - side, False)
        make_left()
        l_copy(lf, lf).wait_recv()
        copies[2].start()

    pl.when(t == 0)(lambda: end_left(0))
    pl.when(t == T - 1)(lambda: end_left(1))
    pl.when((t == 1) | (t == T - 2))(guest_emit)
    loop(0, jnp.where(inner, L, L - 1), emit)

    nsend[1, pl.ds(lf, 1), :] = nsend[1, pl.ds(lf, 1), :] + guest_n[...]
    sums = jnp.sum(nsend[...], axis=2)
    tile[0:1, 0:L] = sums[0:1]
    tile[0:1, L:2 * L] = sums[1:2]

    def n_copy(slot, dst):
        return pltpu.make_async_remote_copy(
            src_ref=tile, dst_ref=nin.at[slot], send_sem=ns, recv_sem=nr,
            device_id={"layer": lax.div(dst, T), "tensor": lax.rem(dst, T)}, device_id_type=MESH)

    loop(1, N, lambda d: n_copy(here, lax.rem(here + d, N)).start())
    pl.when(t == T - 2)(lambda: p_copy(guest_x, final).start())
    pl.when(t == 1)(lambda: q_copy(guest_x, final).start())
    nin[here] = tile[...]

    def sent(ref, sem, axis):
        remote(ref, ref, sem, sem, axis, 0).wait_send()

    most = pl.ds(0, L - 1)
    for ref, sem in ((uall, us), (cb, bs), (vall, xs), (mout, ms), (lall, ls)):
        sent(ref.at[most], sem, "layer")
    pl.when(has_right)(lambda: k_copy(core_out, 0).wait_send())
    pl.when(has_left)(lambda: k_copy(core_out, 1).wait_send())

    pl.when(has_right)(lambda: sent(own, ps, "tensor"))
    pl.when(has_left)(lambda: sent(own, qs, "tensor"))

    def drain_v(c):
        pl.when((c <= t) & has_right)(lambda: sent(vline.at[c], vs.at[0, c], "tensor"))
        pl.when((c >= t) & has_left)(lambda: sent(vline.at[c], vs.at[1, c], "tensor"))

    loop(0, T, drain_v)

    for side, end in ((0, 0), (1, T - 1)):
        @pl.when(t == end)
        def _(side=side):
            for copy in h_copies(side):
                copy.wait_send()

    arrived = remote(nin.at[pl.ds(0, N - 1)], nin.at[pl.ds(0, N - 1)], ns, nr, "layer", 0)
    arrived.wait_recv()
    tot = jnp.sum(nin[...], axis=0)
    fac = jnp.sqrt((tot[:, 0:L] + 1.0) / (tot[:, L:2 * L] + 1.0))
    factor[...] = jnp.broadcast_to(jnp.transpose(jnp.broadcast_to(fac, (8, L)))[:, 0:1], factor.shape)
    arrived.wait_send()

    def scale(l, rows):
        raw[l] = (rows.astype(F32) * factor[pl.ds(l, 1), 0:1]).astype(BF16)

    def rescale(d):
        l = layer_of(d)
        scale(l, raw[l])

    loop(0, jnp.where(inner, L, L - 1), rescale)

    @pl.when(t == T - 1)
    def _():
        p_copy(own.at[final], final).wait_recv()
        scale(lf, pin[final])

    @pl.when(t == 0)
    def _():
        q_copy(own.at[final], final).wait_recv()
        scale(lf, qin[final])


def solution(mesh):
    L, T = mesh.shape["layer"], mesh.shape["tensor"]
    NP = L // T

    def body(gradient, row_basis, column_basis, row_eigen, column_eigen, row_escape, column_escape):
        _, r, W = gradient.shape
        _, Cr, K = column_basis.shape
        vmem = pl.BlockSpec(memory_space=pltpu.VMEM)
        hbm = pl.BlockSpec(memory_space=pl.ANY)
        chunk = pltpu.VMEM((L, K, W), BF16)
        small = pltpu.VMEM((L, r, K), BF16)
        sem = pltpu.SemaphoreType.DMA
        rows = pl.pallas_call(
            functools.partial(kernel, L, T, NP),
            out_shape=pltpu.VMEM((L, r, W), BF16),
            in_specs=[hbm] * 7,
            out_specs=vmem,
            scratch_shapes=[
                pltpu.VMEM((L, r, W), BF16),
                pltpu.VMEM((r, K), BF16),
                pltpu.VMEM((1, K), F32), pltpu.VMEM((1, K), F32),
                pltpu.VMEM((1, 1), F32), pltpu.VMEM((1, 1), F32),
                small,
                pltpu.VMEM((L, W, K), BF16),
                pltpu.VMEM((T, NP, Cr // NP, K), BF16),
                chunk, chunk, chunk,
                small, small,
                pltpu.VMEM((r, K), F32),
                small,
                pltpu.VMEM((K, K), BF16),
                pltpu.VMEM((2, K, K), BF16),
                pltpu.VMEM((2, K, K), BF16),
                pltpu.VMEM((L, 8, K), F32),
                pltpu.VMEM((r, W), BF16),
                pltpu.VMEM((r, K), BF16),
                pltpu.VMEM((r, K), BF16),
                pltpu.VMEM((r, W), BF16),
                pltpu.VMEM((1, 128), F32),
                pltpu.VMEM((2, L, 128), F32),
                pltpu.VMEM((1, 128), F32),
                pltpu.VMEM((L * T, 1, 128), F32),
                pltpu.VMEM((L, 128), F32),
                sem, sem((L,)),
                sem, sem((L,)),
                sem((2, T)), sem((T, NP)),
                sem, sem((L,)),
                sem, sem,
                sem((2,)), sem((2,)),
                sem, sem((L,)),
                sem, sem((L,)),
                sem, sem((L,)),
                sem, sem,
                sem((3,)), sem((3,)),
                sem, sem((NP,)), sem((5,)),
            ],
            compiler_params=pltpu.CompilerParams(
                collective_id=0, has_side_effects=True, vmem_limit_bytes=67043328 - 2 * L * r * W - 256 * 1024),
        )(gradient, row_basis[0], column_basis[0], row_eigen, column_eigen,
          row_escape[:, None], column_escape[:, None])
        return rows

    in_specs = (
        P(None, "tensor", "layer"),
        P("layer", "tensor", None),
        P("layer", "tensor", None),
        P("layer", None),
        P("layer", None),
        P("layer"),
        P("layer"),
    )
    out_specs = P(None, "tensor", "layer")
    return jax.shard_map(body, mesh=mesh, in_specs=in_specs, out_specs=out_specs, check_vma=False)
```

```python
import functools

import jax
import jax.numpy as jnp
from jax import lax
from jax.experimental import pallas as pl
from jax.experimental.pallas import tpu as pltpu
from jax.sharding import PartitionSpec as P

MESH = pl.DeviceIdType.MESH
F32 = jnp.float32
BF16 = jnp.bfloat16


def remote(src, dst, send, recv, axis, index):
    return pltpu.make_async_remote_copy(
        src_ref=src,
        dst_ref=dst,
        send_sem=send,
        recv_sem=recv,
        device_id={axis: index},
        device_id_type=MESH,
    )


def loop(lo, hi, fn):
    def step(i, carry):
        fn(i)
        return carry

    lax.fori_loop(lo, hi, step, 0)


def dot(a, b, dims=((1,), (0,))):
    return lax.dot_general(a, b, (dims, ((), ())), preferred_element_type=F32)


def quarter(x):
    return lax.rsqrt(jnp.sqrt(x))


def lanes(x):
    s = jnp.sum(x * x, axis=0, keepdims=True)
    out = s[:, 0:128]
    for k in range(1, x.shape[1] // 128):
        out = out + s[:, k * 128:(k + 1) * 128]
    return out


def kernel(
    L, T, NP,
    g_hbm, u_hbm, cols_hbm, reig_hbm, ceig_hbm, resc_hbm, cesc_hbm,
    raw,
    g, u, reig, ceig, resc, cesc, uall, vall, vline, own, pin, qin, mout, mpal, mi, mid, lall, core_out, core_in, core_sum, cb,
    guest_g, guest_u, guest_l, guest_x, guest_n, nsend, tile, nin, factor,
    us, ur, bs, br, vs, vr, xs, xr, ms, mr, ks, kr, ls, lr, ps, pr, qs, qr, ns, nr, hs, hr, zs, zr, gs, cs, es,
):
    me = lax.axis_index("layer")
    t = lax.axis_index("tensor")
    W = g.shape[2]
    K = u.shape[1]
    right, lft = t + 1, t - 1
    has_right, has_left = t < T - 1, t > 0
    inner = has_right & has_left
    far = jnp.maximum(t, T - 1 - t)
    n_left, n_right = t, T - 1 - t

    here = me * T + t
    N = L * T

    g_in = pltpu.make_async_copy(g_hbm, g, gs)
    small_in = [pltpu.make_async_copy(src, dst, es.at[k]) for k, (src, dst) in enumerate((
        (u_hbm, u), (reig_hbm, reig), (ceig_hbm, ceig), (resc_hbm, resc), (cesc_hbm, cesc)))]

    def cols_in(i):
        return pltpu.make_async_copy(cols_hbm.at[pl.ds(i * W, W)], vline.at[t, i], cs.at[i])

    for i in range(NP):
        cols_in(i).start()

    bits = [1 << b for b in range(L.bit_length() - 1)]

    def masks(k):
        return [mask for mask in range(1, L) if bin(mask).count("1") == k]

    def partner(mask):
        index = me
        for b in bits:
            if mask & b:
                index = index + b - 2 * b * lax.rem(lax.div(me, b), 2)
        return index

    def greet(axis, index):
        pl.semaphore_signal(barrier, inc=1, device_id={axis: index}, device_id_type=MESH)

    barrier = pltpu.get_barrier_semaphore()
    pl.when(has_right)(lambda: greet("tensor", right))
    pl.when(has_left)(lambda: greet("tensor", lft))
    for mask in masks(1):
        greet("layer", partner(mask))
    for copy in small_in:
        copy.start()
    g_in.start()
    for i in range(NP):
        cols_in(i).wait()
    pl.semaphore_wait(barrier, len(bits) + jnp.where(inner, 2, 1))

    def layer_of(d):
        return lax.rem(me + d, L)

    def v_copy(src, c, i, side):
        return remote(src, vline.at[c, i], vs.at[side, c], vr.at[c, i], "tensor",
                      right if side == 0 else lft)

    def x_copy(src, slot, dst):
        return remote(src, vall.at[slot], xs, xr.at[slot], "layer", dst)

    def u_copy(slot, dst):
        return remote(u, uall.at[slot], us, ur.at[slot], "layer", dst)

    def b_copy(slot, dst):
        return remote(cb.at[me], cb.at[slot], bs, br.at[slot], "layer", dst)

    def m_copy(slot, dst):
        return remote(mout.at[dst], mi.at[slot], ms, mr, "layer", dst)

    def l_copy(slot, dst):
        return remote(lall.at[me], lall.at[slot], ls, lr.at[slot], "layer", dst)

    def k_copy(src, side):
        return remote(src, core_in.at[side], ks.at[side], kr.at[side], "tensor", right if side == 0 else lft)

    def p_copy(src, d):
        return remote(src, pin.at[d], ps, pr.at[d], "tensor", right)

    def q_copy(src, d):
        return remote(src, qin.at[d], qs, qr.at[d], "tensor", lft)

    def send_own(i, side):
        v_copy(vline.at[t, i], t, i, side).start()

    def send_half(i, half, side):
        rows = vline.at[t, i, pl.ds(half * (W // 2), W // 2)]
        remote(rows, rows, vs.at[side, t], vr.at[t, i], "tensor", right if side == 0 else lft).start()

    def send_first(side, onward, n):
        @pl.when(onward)
        def _():
            loop(0, jnp.where(n > 0, 1, NP), lambda i: send_own(i, side))
            pl.when((n > 0) & (NP > 1))(lambda: send_half(1, 0, side))

    send_first(0, has_right, n_left)
    send_first(1, has_left, n_right)
    for copy in small_in:
        copy.wait()
    tile[...] = jnp.zeros_like(tile)
    row_base = quarter(resc[...])
    column_base = quarter(cesc[...])
    row_coef = quarter(reig[...] + resc[...]) - row_base
    dc = quarter(ceig[...] + cesc[...]) - column_base
    cb[me, 0:1, :] = row_coef * column_base
    cb[me, 1:2, :] = jnp.broadcast_to(row_base * column_base, (1, K))
    cb[me, 2:8, :] = jnp.broadcast_to(row_coef, (6, K))
    uall[me] = u[...]

    def send_basis(mask):
        dst = partner(mask)
        u_copy(me, dst).start()
        b_copy(me, dst).start()

    def take_basis(mask):
        src = partner(mask)
        u_copy(src, src).wait_recv()

    for mask in masks(1):
        send_basis(mask)

    def spread(c, i):
        dst = c * NP + i
        pl.when(dst != me)(lambda: x_copy(vline.at[c, i], me, dst).start())

        @pl.when(dst == me)
        def _():
            vall[me] = vline[c, i]

    @pl.when(t == 0)
    def _():
        loop(0, L, lambda d: pin.__setitem__(d, jnp.zeros(pin.shape[1:], BF16)))

    @pl.when(t == T - 1)
    def _():
        loop(0, L, lambda d: qin.__setitem__(d, jnp.zeros(qin.shape[1:], BF16)))

    def project(d):
        l = layer_of(d)

        @pl.when(d > 0)
        def _():
            b_copy(l, l).wait_recv()

        block = g[l]
        own[d] = dot(uall[l], block, ((0,), (0,))).astype(BF16)
        nsend[0, pl.ds(l, 1), :] = lanes(block.astype(F32))

    g_in.wait()
    project(0)
    for k in range(1, len(bits)):
        for mask in masks(k):
            take_basis(mask)
        for mask in masks(k + 1):
            send_basis(mask)

    def end_send(d):
        @pl.when((d >= 0) & (d < L))
        def _():
            pl.when(t == 0)(lambda: p_copy(own.at[d], d).start())
            pl.when(t == T - 1)(lambda: q_copy(own.at[d], d).start())

    def core_pass(side, onward):
        k_copy(core_out, side).wait_recv()

        @pl.when(onward)
        def _():
            core_sum[side] = (core_in[side].astype(F32) + core_out[...].astype(F32)).astype(BF16)
            k_copy(core_sum.at[side], side).start()

    def forward(s, tau, copy, buf, side):
        d = s - NP * tau - 1
        ok = (d >= 0) & (d < L) & inner
        pl.when(ok)(lambda: copy(own.at[0], d).wait_recv())
        pl.when(inner & (s == at_core_end + tau))(lambda: core_pass(side, True))

        @pl.when(ok)
        def _():
            buf[d] = (buf[d].astype(F32) + own[d].astype(F32)).astype(BF16)
            pl.when((d < L - 1) | (tau < T - 2))(lambda: copy(buf.at[d], d).start())

    def relay(s, n, way, side, onward):
        near = jnp.maximum(n, 1)
        i, h = lax.div(s - 1, near), lax.rem(s - 1, near) + 1
        c = t + way * h

        @pl.when(s <= NP * n)
        def _():
            v_copy(vline.at[c, i], c, i, side).wait_recv()
            pl.when(onward)(lambda: v_copy(vline.at[c, i], c, i, side).start())
            pl.when(onward & (h == 1) & (i + 1 < NP))(lambda: send_half(i + 1, 1, side))
            pl.when(onward & (h == n) & (i + 2 < NP))(lambda: send_half(i + 2, 0, side))
            spread(c, i)

    def middle(d):
        l = layer_of(d)
        pl.when(d > 0)(lambda: x_copy(vall.at[l], l, l).wait_recv())
        mout[l] = dot(g[l], vall[l]).astype(BF16)
        pl.when(lax.rem(l, 2) != lax.rem(me, 2))(lambda: z_copy(l).start())

    def z_copy(l):
        pal = me + 1 - 2 * lax.rem(me, 2)
        return remote(mout.at[l], mpal.at[lax.div(l, 2)], zs, zr, "layer", pal)

    half = L // 2

    def add_pairs():
        remote(mpal, mpal, zs, zr, "layer", me).wait_recv()

        def one(j):
            l = lax.rem(me, 2) + 2 * j
            both = (mout[l].astype(F32) + mpal[j].astype(F32)).astype(BF16)

            @pl.when(l == me)
            def _():
                mi[j] = both

            @pl.when(l != me)
            def _():
                mout[l] = both
                m_copy(lax.div(me, 2), l).start()

        loop(0, half, one)

    def gather_middle():
        add_pairs()
        remote(mout.at[pl.ds(0, half - 1)], mi.at[pl.ds(0, half - 1)], ms, mr, "layer", me).wait_recv()
        mid[...] = mi[0].astype(F32)

        def add(j):
            mid[...] += mi[j].astype(F32)

        loop(1, half, add)
        core_out[...] = dot(u[...], mid[...].astype(BF16), ((0,), (0,))).astype(BF16)

        @pl.when(t == 0)
        def _():
            core_in[0] = jnp.zeros(core_out.shape, BF16)
            k_copy(core_out, 0).start()

        @pl.when(t == T - 1)
        def _():
            core_in[1] = jnp.zeros(core_out.shape, BF16)
            k_copy(core_out, 1).start()

    def make_left():
        core = core_in[0].astype(F32) + core_in[1].astype(F32) + core_out[...].astype(F32)
        core = (core * jnp.transpose(cb[me])[:, 2:3]).astype(BF16)
        mixed = row_base * mid[...] + dot(u[...], core)
        lall[me] = (mixed * dc).astype(BF16)
        loop(1, L, lambda d: l_copy(me, lax.rem(me + d, L)).start())

    sign = jnp.where(inner, -1.0, 1.0).astype(F32)

    def pushed(d):
        total = pin[d].astype(F32) + qin[d].astype(F32) + sign * own[d].astype(F32)
        return (total * jnp.transpose(cb[layer_of(d)])[:, 0:1]).astype(BF16)

    def update(l, block, basis, scaled, left):
        x = cb[l, 1:2, 0:1] * block.astype(F32)
        x = x + dot(basis, scaled)
        return x + dot(left, vall[l], ((1,), (1,)))

    def emit(d):
        l = layer_of(d)
        pl.when(d > 0)(lambda: l_copy(l, l).wait_recv())
        pl.when(t == T - 1)(lambda: p_copy(own.at[d], d).wait_recv())
        pl.when(t == 0)(lambda: q_copy(own.at[d], d).wait_recv())
        x = update(l, g[l], uall[l], pushed(d), lall[l])
        raw[l] = x.astype(BF16)
        nsend[1, pl.ds(l, 1), :] = lanes(x)

    final = L - 1
    lf = layer_of(final)

    def h_copies(side):
        to = lax.rem(t + (1 if side == 0 else T - 1), T)
        return [
            remote(src, dst, hs.at[k], hr.at[k], "tensor", to)
            for k, (src, dst) in enumerate(((g.at[lf], guest_g), (uall.at[lf], guest_u), (lall.at[lf], guest_l)))]

    def guest_emit():
        for copy in h_copies(0):
            copy.wait_recv()
        x = update(lf, guest_g[...], guest_u[...], pushed(final), guest_l[...])
        guest_x[...] = x.astype(BF16)
        guest_n[...] = lanes(x)

    blk = lax.rem(me, NP)
    home = lax.div(me, NP)
    dist = jnp.abs(t - home)
    third = -(-L // 3)
    first = jnp.where(dist == 0, 2 * blk + 4, blk * jnp.where(home < t, n_left, n_right) + dist + 2)
    at_core = NP * far + 2
    at_core_end = NP * (T - 1) + 2
    last = max(NP * (T - 2) + L, at_core_end + T - 2, NP * (T - 1) + 2, 2 * NP + 2)

    def step(s):
        relay(s, n_left, -1, 0, has_right)
        relay(s, n_right, 1, 1, has_left)
        pl.when(s == 1)(lambda: loop(0, NP, lambda i: spread(t, i)))
        pl.when(s < L)(lambda: end_send(s - 1))
        pl.when(s == 1)(lambda: take_basis(L - 1))
        loop(jnp.clip(third * (s - 1) + 1, 1, L), jnp.clip(third * s + 1, 1, L), project)
        forward(s, t, p_copy, pin, 0)
        forward(s, T - 1 - t, q_copy, qin, 1)
        loop(jnp.where(s == first, 0, L), L, middle)

        @pl.when(s == at_core)
        def _():
            gather_middle()
            end_send(L - 1)

        pl.when(inner & (s == at_core_end + T - 2))(make_left)

    guest_n[...] = jnp.zeros_like(guest_n)
    nsend[1, pl.ds(lf, 1), :] = jnp.zeros((1, 128), F32)
    loop(1, last + 1, step)

    def end_left(side):
        copies = h_copies(side)
        copies[0].start()
        copies[1].start()
        core_pass(1 - side, False)
        make_left()
        l_copy(lf, lf).wait_recv()
        copies[2].start()

    pl.when(t == 0)(lambda: end_left(0))
    pl.when(t == T - 1)(lambda: end_left(1))
    pl.when((t == 1) | (t == T - 2))(guest_emit)
    loop(0, jnp.where(inner, L, L - 1), emit)

    nsend[1, pl.ds(lf, 1), :] = nsend[1, pl.ds(lf, 1), :] + guest_n[...]
    sums = jnp.sum(nsend[...], axis=2)
    tile[0:1, 0:L] = sums[0:1]
    tile[0:1, L:2 * L] = sums[1:2]

    def n_copy(slot, dst):
        return pltpu.make_async_remote_copy(
            src_ref=tile, dst_ref=nin.at[slot], send_sem=ns, recv_sem=nr,
            device_id={"layer": lax.div(dst, T), "tensor": lax.rem(dst, T)}, device_id_type=MESH)

    loop(1, N, lambda d: n_copy(here, lax.rem(here + d, N)).start())
    pl.when(t == T - 2)(lambda: p_copy(guest_x, final).start())
    pl.when(t == 1)(lambda: q_copy(guest_x, final).start())
    nin[here] = tile[...]

    def sent(ref, sem, axis):
        remote(ref, ref, sem, sem, axis, 0).wait_send()

    most = pl.ds(0, L - 1)
    for ref, sem in ((uall, us), (cb, bs), (vall, xs), (lall, ls)):
        sent(ref.at[most], sem, "layer")
    sent(mout.at[pl.ds(0, half - 1)], ms, "layer")
    sent(mpal, zs, "layer")
    pl.when(has_right)(lambda: k_copy(core_out, 0).wait_send())
    pl.when(has_left)(lambda: k_copy(core_out, 1).wait_send())

    pl.when(has_right)(lambda: sent(own, ps, "tensor"))
    pl.when(has_left)(lambda: sent(own, qs, "tensor"))

    def drain_v(c):
        pl.when((c <= t) & has_right)(lambda: sent(vline.at[c], vs.at[0, c], "tensor"))
        pl.when((c >= t) & has_left)(lambda: sent(vline.at[c], vs.at[1, c], "tensor"))

    loop(0, T, drain_v)

    for side, end in ((0, 0), (1, T - 1)):
        @pl.when(t == end)
        def _(side=side):
            for copy in h_copies(side):
                copy.wait_send()

    arrived = remote(nin.at[pl.ds(0, N - 1)], nin.at[pl.ds(0, N - 1)], ns, nr, "layer", 0)
    arrived.wait_recv()
    tot = jnp.sum(nin[...], axis=0)
    fac = jnp.sqrt((tot[:, 0:L] + 1.0) / (tot[:, L:2 * L] + 1.0))
    factor[...] = jnp.broadcast_to(jnp.transpose(jnp.broadcast_to(fac, (8, L)))[:, 0:1], factor.shape)
    arrived.wait_send()

    def scale(l, rows):
        raw[l] = (rows.astype(F32) * factor[pl.ds(l, 1), 0:1]).astype(BF16)

    def rescale(d):
        l = layer_of(d)
        scale(l, raw[l])

    loop(0, jnp.where(inner, L, L - 1), rescale)

    @pl.when(t == T - 1)
    def _():
        p_copy(own.at[final], final).wait_recv()
        scale(lf, pin[final])

    @pl.when(t == 0)
    def _():
        q_copy(own.at[final], final).wait_recv()
        scale(lf, qin[final])


def solution(mesh):
    L, T = mesh.shape["layer"], mesh.shape["tensor"]
    NP = L // T

    def body(gradient, row_basis, column_basis, row_eigen, column_eigen, row_escape, column_escape):
        _, r, W = gradient.shape
        _, Cr, K = column_basis.shape
        vmem = pl.BlockSpec(memory_space=pltpu.VMEM)
        hbm = pl.BlockSpec(memory_space=pl.ANY)
        chunk = pltpu.VMEM((L, K, W), BF16)
        small = pltpu.VMEM((L, r, K), BF16)
        sem = pltpu.SemaphoreType.DMA
        rows = pl.pallas_call(
            functools.partial(kernel, L, T, NP),
            out_shape=pltpu.VMEM((L, r, W), BF16),
            in_specs=[hbm] * 7,
            out_specs=vmem,
            scratch_shapes=[
                pltpu.VMEM((L, r, W), BF16),
                pltpu.VMEM((r, K), BF16),
                pltpu.VMEM((1, K), F32), pltpu.VMEM((1, K), F32),
                pltpu.VMEM((1, 1), F32), pltpu.VMEM((1, 1), F32),
                small,
                pltpu.VMEM((L, W, K), BF16),
                pltpu.VMEM((T, NP, Cr // NP, K), BF16),
                chunk, chunk, chunk,
                small,
                pltpu.VMEM((L // 2, r, K), BF16),
                pltpu.VMEM((L // 2, r, K), BF16),
                pltpu.VMEM((r, K), F32),
                small,
                pltpu.VMEM((K, K), BF16),
                pltpu.VMEM((2, K, K), BF16),
                pltpu.VMEM((2, K, K), BF16),
                pltpu.VMEM((L, 8, K), F32),
                pltpu.VMEM((r, W), BF16),
                pltpu.VMEM((r, K), BF16),
                pltpu.VMEM((r, K), BF16),
                pltpu.VMEM((r, W), BF16),
                pltpu.VMEM((1, 128), F32),
                pltpu.VMEM((2, L, 128), F32),
                pltpu.VMEM((1, 128), F32),
                pltpu.VMEM((L * T, 1, 128), F32),
                pltpu.VMEM((L, 128), F32),
                sem, sem((L,)),
                sem, sem((L,)),
                sem((2, T)), sem((T, NP)),
                sem, sem((L,)),
                sem, sem,
                sem((2,)), sem((2,)),
                sem, sem((L,)),
                sem, sem((L,)),
                sem, sem((L,)),
                sem, sem,
                sem((3,)), sem((3,)),
                sem, sem,
                sem, sem((NP,)), sem((5,)),
            ],
            compiler_params=pltpu.CompilerParams(
                collective_id=0, has_side_effects=True, vmem_limit_bytes=67043328 - 2 * L * r * W - 256 * 1024),
        )(gradient, row_basis[0], column_basis[0], row_eigen, column_eigen,
          row_escape[:, None], column_escape[:, None])
        return rows

    in_specs = (
        P(None, "tensor", "layer"),
        P("layer", "tensor", None),
        P("layer", "tensor", None),
        P("layer", None),
        P("layer", None),
        P("layer"),
        P("layer"),
    )
    out_specs = P(None, "tensor", "layer")
    return jax.shard_map(body, mesh=mesh, in_specs=in_specs, out_specs=out_specs, check_vma=False)
```

```python
import functools

import jax
import jax.numpy as jnp
from jax import lax
from jax.experimental import pallas as pl
from jax.experimental.pallas import tpu as pltpu
from jax.sharding import PartitionSpec as P

MESH = pl.DeviceIdType.MESH
F32 = jnp.float32
BF16 = jnp.bfloat16


def remote(src, dst, send, recv, axis, index):
    return pltpu.make_async_remote_copy(
        src_ref=src,
        dst_ref=dst,
        send_sem=send,
        recv_sem=recv,
        device_id={axis: index},
        device_id_type=MESH,
    )


def loop(lo, hi, fn):
    def step(i, carry):
        fn(i)
        return carry

    lax.fori_loop(lo, hi, step, 0)


def dot(a, b, dims=((1,), (0,))):
    return lax.dot_general(a, b, (dims, ((), ())), preferred_element_type=F32)


def quarter(x):
    return lax.rsqrt(jnp.sqrt(x))


def lanes(x):
    s = jnp.sum(x * x, axis=0, keepdims=True)
    out = s[:, 0:128]
    for k in range(1, x.shape[1] // 128):
        out = out + s[:, k * 128:(k + 1) * 128]
    return out


def kernel(
    L, T, NP,
    g_hbm, u_hbm, cols_hbm, reig_hbm, ceig_hbm, resc_hbm, cesc_hbm,
    raw,
    g, u, reig, ceig, resc, cesc, uall, vall, vline, own, pin, qin, mout, mpal, mi, mid, lall, core_out, core_in, core_sum, cb,
    guest_g, guest_u, guest_l, guest_x, guest_n, nsend, tile, nin, factor,
    us, ur, bs, br, vs, vr, xs, xr, ms, mr, ks, kr, ls, lr, ps, pr, qs, qr, ns, nr, hs, hr, zs, zr, gs, cs, es,
):
    me = lax.axis_index("layer")
    t = lax.axis_index("tensor")
    W = g.shape[2]
    K = u.shape[1]
    right, lft = t + 1, t - 1
    has_right, has_left = t < T - 1, t > 0
    inner = has_right & has_left
    far = jnp.maximum(t, T - 1 - t)
    n_left, n_right = t, T - 1 - t

    here = me * T + t
    N = L * T

    g_in = pltpu.make_async_copy(g_hbm, g, gs)
    small_in = [pltpu.make_async_copy(src, dst, es.at[k]) for k, (src, dst) in enumerate((
        (u_hbm, u), (reig_hbm, reig), (ceig_hbm, ceig), (resc_hbm, resc), (cesc_hbm, cesc)))]

    def cols_in(i):
        return pltpu.make_async_copy(cols_hbm.at[pl.ds(i * W, W)], vline.at[t, i], cs.at[i])

    for i in range(NP):
        cols_in(i).start()

    bits = [1 << b for b in range(L.bit_length() - 1)]

    def masks(k):
        return [mask for mask in range(1, L) if bin(mask).count("1") == k]

    def partner(mask):
        index = me
        for b in bits:
            if mask & b:
                index = index + b - 2 * b * lax.rem(lax.div(me, b), 2)
        return index

    def greet(axis, index):
        pl.semaphore_signal(barrier, inc=1, device_id={axis: index}, device_id_type=MESH)

    barrier = pltpu.get_barrier_semaphore()
    pl.when(has_right)(lambda: greet("tensor", right))
    pl.when(has_left)(lambda: greet("tensor", lft))
    for mask in masks(1):
        greet("layer", partner(mask))
    for copy in small_in:
        copy.start()
    g_in.start()
    cols_in(0).wait()
    pl.semaphore_wait(barrier, len(bits) + jnp.where(inner, 2, 1))

    def layer_of(d):
        return lax.rem(me + d, L)

    def v_copy(src, c, i, side):
        return remote(src, vline.at[c, i], vs.at[side, c], vr.at[c, i], "tensor",
                      right if side == 0 else lft)

    def x_copy(src, slot, dst):
        return remote(src, vall.at[slot], xs, xr.at[slot], "layer", dst)

    def u_copy(slot, dst):
        return remote(u, uall.at[slot], us, ur.at[slot], "layer", dst)

    def b_copy(slot, dst):
        return remote(cb.at[me], cb.at[slot], bs, br.at[slot], "layer", dst)

    def m_copy(slot, dst):
        return remote(mout.at[dst], mi.at[slot], ms, mr, "layer", dst)

    def l_copy(slot, dst):
        return remote(lall.at[me], lall.at[slot], ls, lr.at[slot], "layer", dst)

    def k_copy(src, side):
        return remote(src, core_in.at[side], ks.at[side], kr.at[side], "tensor", right if side == 0 else lft)

    def p_copy(src, d):
        return remote(src, pin.at[d], ps, pr.at[d], "tensor", right)

    def q_copy(src, d):
        return remote(src, qin.at[d], qs, qr.at[d], "tensor", lft)

    def send_own(i, side):
        v_copy(vline.at[t, i], t, i, side).start()

    def send_half(i, half, side):
        rows = vline.at[t, i, pl.ds(half * (W // 2), W // 2)]
        remote(rows, rows, vs.at[side, t], vr.at[t, i], "tensor", right if side == 0 else lft).start()

    def send_first(side, onward, n):
        @pl.when(onward)
        def _():
            loop(1, jnp.where(n > 0, 1, NP), lambda i: send_own(i, side))
            pl.when((n > 0) & (NP > 1))(lambda: send_half(1, 0, side))

    pl.when(has_right)(lambda: send_own(0, 0))
    pl.when(has_left)(lambda: send_own(0, 1))
    for i in range(1, NP):
        cols_in(i).wait()
    send_first(0, has_right, n_left)
    send_first(1, has_left, n_right)
    for copy in small_in:
        copy.wait()
    tile[...] = jnp.zeros_like(tile)
    row_base = quarter(resc[...])
    column_base = quarter(cesc[...])
    row_coef = quarter(reig[...] + resc[...]) - row_base
    dc = quarter(ceig[...] + cesc[...]) - column_base
    cb[me, 0:1, :] = row_coef * column_base
    cb[me, 1:2, :] = jnp.broadcast_to(row_base * column_base, (1, K))
    cb[me, 2:8, :] = jnp.broadcast_to(row_coef, (6, K))
    uall[me] = u[...]

    def send_basis(mask):
        dst = partner(mask)
        u_copy(me, dst).start()
        b_copy(me, dst).start()

    def take_basis(mask):
        src = partner(mask)
        u_copy(src, src).wait_recv()

    for mask in masks(1):
        send_basis(mask)

    def spread(c, i):
        dst = c * NP + i
        pl.when(dst != me)(lambda: x_copy(vline.at[c, i], me, dst).start())

        @pl.when(dst == me)
        def _():
            vall[me] = vline[c, i]

    @pl.when(t == 0)
    def _():
        loop(0, L, lambda d: pin.__setitem__(d, jnp.zeros(pin.shape[1:], BF16)))

    @pl.when(t == T - 1)
    def _():
        loop(0, L, lambda d: qin.__setitem__(d, jnp.zeros(qin.shape[1:], BF16)))

    def project(d):
        l = layer_of(d)

        @pl.when(d > 0)
        def _():
            b_copy(l, l).wait_recv()

        block = g[l]
        own[d] = dot(uall[l], block, ((0,), (0,))).astype(BF16)
        nsend[0, pl.ds(l, 1), :] = lanes(block.astype(F32))

    g_in.wait()
    project(0)
    for k in range(1, len(bits)):
        for mask in masks(k):
            take_basis(mask)
        for mask in masks(k + 1):
            send_basis(mask)

    def end_send(d):
        @pl.when((d >= 0) & (d < L))
        def _():
            pl.when(t == 0)(lambda: p_copy(own.at[d], d).start())
            pl.when(t == T - 1)(lambda: q_copy(own.at[d], d).start())

    def core_pass(side, onward):
        k_copy(core_out, side).wait_recv()

        @pl.when(onward)
        def _():
            core_sum[side] = (core_in[side].astype(F32) + core_out[...].astype(F32)).astype(BF16)
            k_copy(core_sum.at[side], side).start()

    def forward(s, tau, copy, buf, side):
        d = s - NP * tau - 1
        ok = (d >= 0) & (d < L) & inner
        pl.when(ok)(lambda: copy(own.at[0], d).wait_recv())
        pl.when(inner & (s == at_core_end + tau))(lambda: core_pass(side, True))

        @pl.when(ok)
        def _():
            buf[d] = (buf[d].astype(F32) + own[d].astype(F32)).astype(BF16)
            pl.when((d < L - 1) | (tau < T - 2))(lambda: copy(buf.at[d], d).start())

    def relay(s, n, way, side, onward):
        near = jnp.maximum(n, 1)
        i, h = lax.div(s - 1, near), lax.rem(s - 1, near) + 1
        c = t + way * h

        @pl.when(s <= NP * n)
        def _():
            v_copy(vline.at[c, i], c, i, side).wait_recv()
            pl.when(onward)(lambda: v_copy(vline.at[c, i], c, i, side).start())
            pl.when(onward & (h == 1) & (i + 1 < NP))(lambda: send_half(i + 1, 1, side))
            pl.when(onward & (h == n) & (i + 2 < NP))(lambda: send_half(i + 2, 0, side))
            spread(c, i)

    def middle(d):
        l = layer_of(d)
        pl.when(d > 0)(lambda: x_copy(vall.at[l], l, l).wait_recv())
        mout[l] = dot(g[l], vall[l]).astype(BF16)
        pl.when(lax.rem(l, 2) != lax.rem(me, 2))(lambda: z_copy(l).start())

    def z_copy(l):
        pal = me + 1 - 2 * lax.rem(me, 2)
        return remote(mout.at[l], mpal.at[lax.div(l, 2)], zs, zr, "layer", pal)

    half = L // 2

    def add_pairs():
        remote(mpal, mpal, zs, zr, "layer", me).wait_recv()

        def one(j):
            l = lax.rem(me, 2) + 2 * j
            both = (mout[l].astype(F32) + mpal[j].astype(F32)).astype(BF16)

            @pl.when(l == me)
            def _():
                mi[j] = both

            @pl.when(l != me)
            def _():
                mout[l] = both
                m_copy(lax.div(me, 2), l).start()

        loop(0, half, one)

    def gather_middle():
        add_pairs()
        remote(mout.at[pl.ds(0, half - 1)], mi.at[pl.ds(0, half - 1)], ms, mr, "layer", me).wait_recv()
        mid[...] = mi[0].astype(F32)

        def add(j):
            mid[...] += mi[j].astype(F32)

        loop(1, half, add)
        core_out[...] = dot(u[...], mid[...].astype(BF16), ((0,), (0,))).astype(BF16)

        @pl.when(t == 0)
        def _():
            core_in[0] = jnp.zeros(core_out.shape, BF16)
            k_copy(core_out, 0).start()

        @pl.when(t == T - 1)
        def _():
            core_in[1] = jnp.zeros(core_out.shape, BF16)
            k_copy(core_out, 1).start()

    def make_left():
        core = core_in[0].astype(F32) + core_in[1].astype(F32) + core_out[...].astype(F32)
        core = (core * jnp.transpose(cb[me])[:, 2:3]).astype(BF16)
        mixed = row_base * mid[...] + dot(u[...], core)
        lall[me] = (mixed * dc).astype(BF16)
        loop(1, L, lambda d: l_copy(me, lax.rem(me + d, L)).start())

    sign = jnp.where(inner, -1.0, 1.0).astype(F32)

    def pushed(d):
        total = pin[d].astype(F32) + qin[d].astype(F32) + sign * own[d].astype(F32)
        return (total * jnp.transpose(cb[layer_of(d)])[:, 0:1]).astype(BF16)

    def update(l, block, basis, scaled, left):
        x = cb[l, 1:2, 0:1] * block.astype(F32)
        x = x + dot(basis, scaled)
        return x + dot(left, vall[l], ((1,), (1,)))

    def emit(d):
        l = layer_of(d)
        pl.when(d > 0)(lambda: l_copy(l, l).wait_recv())
        pl.when(t == T - 1)(lambda: p_copy(own.at[d], d).wait_recv())
        pl.when(t == 0)(lambda: q_copy(own.at[d], d).wait_recv())
        x = update(l, g[l], uall[l], pushed(d), lall[l])
        raw[l] = x.astype(BF16)
        nsend[1, pl.ds(l, 1), :] = lanes(x)

    final = L - 1
    lf = layer_of(final)

    def h_copies(side):
        to = lax.rem(t + (1 if side == 0 else T - 1), T)
        return [
            remote(src, dst, hs.at[k], hr.at[k], "tensor", to)
            for k, (src, dst) in enumerate(((g.at[lf], guest_g), (uall.at[lf], guest_u), (lall.at[lf], guest_l)))]

    def guest_emit():
        for copy in h_copies(0):
            copy.wait_recv()
        x = update(lf, guest_g[...], guest_u[...], pushed(final), guest_l[...])
        guest_x[...] = x.astype(BF16)
        guest_n[...] = lanes(x)

    blk = lax.rem(me, NP)
    home = lax.div(me, NP)
    dist = jnp.abs(t - home)
    third = -(-L // 3)
    first = jnp.where(dist == 0, 2 * blk + 4, blk * jnp.where(home < t, n_left, n_right) + dist + 2)
    at_core = NP * far + 2
    at_core_end = NP * (T - 1) + 2
    last = max(NP * (T - 2) + L, at_core_end + T - 2, NP * (T - 1) + 2, 2 * NP + 2)

    def step(s):
        relay(s, n_left, -1, 0, has_right)
        relay(s, n_right, 1, 1, has_left)
        pl.when(s == 1)(lambda: loop(0, NP, lambda i: spread(t, i)))
        pl.when(s < L)(lambda: end_send(s - 1))
        pl.when(s == 1)(lambda: take_basis(L - 1))
        loop(jnp.clip(third * (s - 1) + 1, 1, L), jnp.clip(third * s + 1, 1, L), project)
        forward(s, t, p_copy, pin, 0)
        forward(s, T - 1 - t, q_copy, qin, 1)
        loop(jnp.where(s == first, 0, L), L, middle)

        @pl.when(s == at_core)
        def _():
            gather_middle()
            end_send(L - 1)

        pl.when(inner & (s == at_core_end + T - 2))(make_left)

    guest_n[...] = jnp.zeros_like(guest_n)
    nsend[1, pl.ds(lf, 1), :] = jnp.zeros((1, 128), F32)
    loop(1, last + 1, step)

    def end_left(side):
        copies = h_copies(side)
        copies[0].start()
        copies[1].start()
        core_pass(1 - side, False)
        make_left()
        l_copy(lf, lf).wait_recv()
        copies[2].start()

    pl.when(t == 0)(lambda: end_left(0))
    pl.when(t == T - 1)(lambda: end_left(1))
    pl.when((t == 1) | (t == T - 2))(guest_emit)
    loop(0, jnp.where(inner, L, L - 1), emit)

    nsend[1, pl.ds(lf, 1), :] = nsend[1, pl.ds(lf, 1), :] + guest_n[...]
    sums = jnp.sum(nsend[...], axis=2)
    tile[0:1, 0:L] = sums[0:1]
    tile[0:1, L:2 * L] = sums[1:2]

    def n_copy(slot, dst):
        return pltpu.make_async_remote_copy(
            src_ref=tile, dst_ref=nin.at[slot], send_sem=ns, recv_sem=nr,
            device_id={"layer": lax.div(dst, T), "tensor": lax.rem(dst, T)}, device_id_type=MESH)

    loop(1, N, lambda d: n_copy(here, lax.rem(here + d, N)).start())
    pl.when(t == T - 2)(lambda: p_copy(guest_x, final).start())
    pl.when(t == 1)(lambda: q_copy(guest_x, final).start())
    nin[here] = tile[...]

    def sent(ref, sem, axis):
        remote(ref, ref, sem, sem, axis, 0).wait_send()

    most = pl.ds(0, L - 1)
    for ref, sem in ((uall, us), (cb, bs), (vall, xs), (lall, ls)):
        sent(ref.at[most], sem, "layer")
    sent(mout.at[pl.ds(0, half - 1)], ms, "layer")
    sent(mpal, zs, "layer")
    pl.when(has_right)(lambda: k_copy(core_out, 0).wait_send())
    pl.when(has_left)(lambda: k_copy(core_out, 1).wait_send())

    pl.when(has_right)(lambda: sent(own, ps, "tensor"))
    pl.when(has_left)(lambda: sent(own, qs, "tensor"))

    def drain_v(c):
        pl.when((c <= t) & has_right)(lambda: sent(vline.at[c], vs.at[0, c], "tensor"))
        pl.when((c >= t) & has_left)(lambda: sent(vline.at[c], vs.at[1, c], "tensor"))

    loop(0, T, drain_v)

    for side, end in ((0, 0), (1, T - 1)):
        @pl.when(t == end)
        def _(side=side):
            for copy in h_copies(side):
                copy.wait_send()

    arrived = remote(nin.at[pl.ds(0, N - 1)], nin.at[pl.ds(0, N - 1)], ns, nr, "layer", 0)
    arrived.wait_recv()
    tot = jnp.sum(nin[...], axis=0)
    fac = jnp.sqrt((tot[:, 0:L] + 1.0) / (tot[:, L:2 * L] + 1.0))
    factor[...] = jnp.broadcast_to(jnp.transpose(jnp.broadcast_to(fac, (8, L)))[:, 0:1], factor.shape)
    arrived.wait_send()

    def scale(l, rows):
        raw[l] = (rows.astype(F32) * factor[pl.ds(l, 1), 0:1]).astype(BF16)

    def rescale(d):
        l = layer_of(d)
        scale(l, raw[l])

    loop(0, jnp.where(inner, L, L - 1), rescale)

    @pl.when(t == T - 1)
    def _():
        p_copy(own.at[final], final).wait_recv()
        scale(lf, pin[final])

    @pl.when(t == 0)
    def _():
        q_copy(own.at[final], final).wait_recv()
        scale(lf, qin[final])


def solution(mesh):
    L, T = mesh.shape["layer"], mesh.shape["tensor"]
    NP = L // T

    def body(gradient, row_basis, column_basis, row_eigen, column_eigen, row_escape, column_escape):
        _, r, W = gradient.shape
        _, Cr, K = column_basis.shape
        vmem = pl.BlockSpec(memory_space=pltpu.VMEM)
        hbm = pl.BlockSpec(memory_space=pl.ANY)
        chunk = pltpu.VMEM((L, K, W), BF16)
        small = pltpu.VMEM((L, r, K), BF16)
        sem = pltpu.SemaphoreType.DMA
        rows = pl.pallas_call(
            functools.partial(kernel, L, T, NP),
            out_shape=pltpu.VMEM((L, r, W), BF16),
            in_specs=[hbm] * 7,
            out_specs=vmem,
            scratch_shapes=[
                pltpu.VMEM((L, r, W), BF16),
                pltpu.VMEM((r, K), BF16),
                pltpu.VMEM((1, K), F32), pltpu.VMEM((1, K), F32),
                pltpu.VMEM((1, 1), F32), pltpu.VMEM((1, 1), F32),
                small,
                pltpu.VMEM((L, W, K), BF16),
                pltpu.VMEM((T, NP, Cr // NP, K), BF16),
                chunk, chunk, chunk,
                small,
                pltpu.VMEM((L // 2, r, K), BF16),
                pltpu.VMEM((L // 2, r, K), BF16),
                pltpu.VMEM((r, K), F32),
                small,
                pltpu.VMEM((K, K), BF16),
                pltpu.VMEM((2, K, K), BF16),
                pltpu.VMEM((2, K, K), BF16),
                pltpu.VMEM((L, 8, K), F32),
                pltpu.VMEM((r, W), BF16),
                pltpu.VMEM((r, K), BF16),
                pltpu.VMEM((r, K), BF16),
                pltpu.VMEM((r, W), BF16),
                pltpu.VMEM((1, 128), F32),
                pltpu.VMEM((2, L, 128), F32),
                pltpu.VMEM((1, 128), F32),
                pltpu.VMEM((L * T, 1, 128), F32),
                pltpu.VMEM((L, 128), F32),
                sem, sem((L,)),
                sem, sem((L,)),
                sem((2, T)), sem((T, NP)),
                sem, sem((L,)),
                sem, sem,
                sem((2,)), sem((2,)),
                sem, sem((L,)),
                sem, sem((L,)),
                sem, sem((L,)),
                sem, sem,
                sem((3,)), sem((3,)),
                sem, sem,
                sem, sem((NP,)), sem((5,)),
            ],
            compiler_params=pltpu.CompilerParams(
                collective_id=0, has_side_effects=True, vmem_limit_bytes=67043328 - 2 * L * r * W - 256 * 1024),
        )(gradient, row_basis[0], column_basis[0], row_eigen, column_eigen,
          row_escape[:, None], column_escape[:, None])
        return rows

    in_specs = (
        P(None, "tensor", "layer"),
        P("layer", "tensor", None),
        P("layer", "tensor", None),
        P("layer", None),
        P("layer", None),
        P("layer"),
        P("layer"),
    )
    out_specs = P(None, "tensor", "layer")
    return jax.shard_map(body, mesh=mesh, in_specs=in_specs, out_specs=out_specs, check_vma=False)
```
